256 devices in a mesh: member: 4 (over y, x), lat: 64 (over z, core).
Axes of the slice: x: 2, y: 2, z: 32, core: 2. Of those that a mesh axis runs over, the one named last changes fastest.
The devices are a block of a 4x8x32 slice.
Arguments:
- field: bfloat16 [1536, 1440, 256], P(('member', 'lat')), parts along dimension 0, may hold values from -3000 to 3000
- gain: float32 [256], replicated, may hold values from 0.1 to 1.9
- slot_wave: int32 [384], replicated, may hold values from 0 to 384, as said below
- legendre: bfloat16 [384, 384, 384], P('lat'), may hold values from -0.3125 to 0.3125
- mixing: bfloat16 [384, 2, 256, 256], P('lat'), may hold values from -0.25 to 0.25
Outputs:
- result: bfloat16 [1536, 1440, 256], P(('member', 'lat')), parts along dimension 0
The draws below stay inside these ranges and needn't reach their ends.
There are 4 independent parts, one for each index of `member`. The reference program is written for one: setup_inputs(seed, part) draws one part's arguments, and reference() takes and returns one part's arrays. A program takes and returns all parts, laid end to end along the dimension named above; an argument that names none is the same for every part. Nothing has to cross between parts.
Inputs may be any that keep to these rules, and one draw needn't show every extreme that they name: `slot_wave`: each wavenumber 0 to 383 stands in exactly one slot and every other slot holds 384; slots 2k and 2k+1 of one lat index hold wavenumbers adding up to (4k+2)64 - 1 where both are below 384.
All inputs are finite; a program needn't handle non-finite values.
Results may differ from the reference program's by a relative error of at most 0.0085.
Values may be sent and summed in bfloat16 or wider, within the bound.
A program may use at most 64 MiB of HBM per device.

```python
import math
import jax
import jax.numpy as jnp
from jax import lax

C = 256
NLON = 1440
NLAT = 384
DEG = 384
SLOT_DEV = 6
SLOTS = 384
N_LAT = 64


def draw_field(key, part):
    keys = jax.random.split(key, 3)
    rows = jnp.arange(NLAT, dtype=jnp.float32) / NLAT
    wobble = 0.3 * jax.random.normal(keys[0], (NLAT,), jnp.float32)
    chan = 10.0 ** jax.random.uniform(keys[1], (C,), jnp.float32, 0.0, 1.0)
    base = jnp.clip(jax.random.normal(keys[2], (NLAT, NLON, C), jnp.float32), -6.0, 6.0)
    row_exp = rows + wobble
    row_exp = jnp.clip(row_exp, -0.5, 1.5)
    values = base * (10.0 ** row_exp)[:, None, None] * chan[None, None, :]
    return values.astype(jnp.bfloat16)


def draw_slot_wave(key, part):
    rounds = SLOT_DEV
    pairs = (rounds + 1) // 2
    keys = jax.random.split(jax.random.fold_in(key, 17), pairs)
    perms = jax.vmap(lambda k: jax.random.permutation(k, N_LAT))(keys)
    round_ids = jnp.arange(rounds, dtype=jnp.int32)[:, None]
    places = jnp.arange(N_LAT, dtype=jnp.int32)[None, :]
    chosen = perms[round_ids[:, 0] // 2]
    picks = jnp.where(round_ids % 2 == 0, places, N_LAT - 1 - places)
    owner = jnp.take_along_axis(chosen, jnp.broadcast_to(picks, (rounds, N_LAT)), axis=1)
    wave = round_ids * N_LAT + places
    wave = jnp.where(wave < DEG, wave, DEG)
    slot = owner * SLOT_DEV + round_ids
    table = jnp.zeros((SLOTS,), jnp.int32)
    return table.at[slot.reshape(-1)].set(jnp.broadcast_to(wave, (rounds, N_LAT)).reshape(-1).astype(jnp.int32))


def levels(rng, dims, cuts, smallest, high):
    level, own = 1.0, jax.random.fold_in(rng, 6)
    for dim, shards_of in cuts:
        heights = jnp.exp(jax.random.uniform(jax.random.fold_in(own, dim), (shards_of,), jnp.float32, smallest / len(cuts), high / len(cuts)))
        level = level * jnp.repeat(heights, dims[dim] // shards_of).reshape([-1 if axis == dim else 1 for axis in range(len(dims))])
    return level


def noise(key, shape, scale, reach, cuts=(), kind=jnp.bfloat16):
    result = jax.random.normal(key, shape, jnp.float32) * scale
    if len(cuts) > 0:
        result = levels(key, shape, cuts, -0.22, 0.18) * result
    return jnp.clip(result, min=-reach, max=reach).astype(kind)


def setup_inputs(seed: int = 0, part: int = 0) -> dict:
    key_of = jax.random.split(jax.random.key(seed), 6)
    part_keys = jax.random.split(jax.random.fold_in(key_of[5], part), 6)
    field = draw_field(jax.random.fold_in(jax.random.fold_in(key_of[5], part), 71), part)
    gain = jnp.clip(1.0 + 0.18 * jax.random.normal(key_of[1], (C,), jnp.float32), 0.1, 1.9)
    slot_wave = draw_slot_wave(jax.random.fold_in(key_of[5], 71), part)
    legendre = noise(key_of[3], (SLOTS, DEG, NLAT), NLAT ** -0.5, 0.3125, ((0, 64),))
    mixing = noise(key_of[4], (SLOTS, 2, C, C), (2 * C) ** -0.5, 0.25, ((0, 64),))
    return {"field": field, "gain": gain, "slot_wave": slot_wave, "legendre": legendre, "mixing": mixing}


def phase_tables(waves, width):
    points = jnp.arange(width, dtype=jnp.int32)
    phase = (waves[:, None] * points[None, :] % width).astype(jnp.float32) * (2.0 * math.pi / width)
    return (jnp.cos(phase), jnp.sin(phase))

def block_weight(mixing):
    real_part = mixing[:, 0]
    imag_part = mixing[:, 1]
    upper = jnp.concatenate([real_part, imag_part], axis=2)
    lower = jnp.concatenate([-imag_part, real_part], axis=2)
    return jnp.concatenate([upper, lower], axis=1)

def reference(field, gain, slot_wave, legendre, mixing):
    values = field.astype(jnp.float32)
    mean = lax.optimization_barrier(jnp.mean(values, axis=(0, 1)))
    var = lax.optimization_barrier(jnp.mean((values - mean) ** 2, axis=(0, 1)))
    normed = ((values - mean) * (gain / jnp.sqrt(var + 1e-05))).astype(jnp.bfloat16)
    cosine, sine = phase_tables(slot_wave, NLON)
    forward = jnp.stack([cosine, -sine]).astype(jnp.bfloat16)
    weight_m = jnp.where(slot_wave == 0, 1.0, 2.0).astype(jnp.float32)[:, None]
    inverse = jnp.stack([weight_m * cosine, -weight_m * sine]).astype(jnp.bfloat16)
    inv_root = 1.0 / math.sqrt(NLON)
    spectrum = jnp.einsum('anc,rkn->karc', normed.astype(jnp.float32), forward.astype(jnp.float32)) * inv_root
    spectrum = spectrum.astype(jnp.bfloat16).reshape(SLOTS, NLAT, 2 * C)
    big = block_weight(mixing)
    lat_scale = math.sqrt(NLAT / DEG)
    degrees = jnp.arange(DEG, dtype=jnp.int32)

    def one_slot(items):
        table, spec, weight, wave = items
        coef = jnp.dot(table, spec, preferred_element_type=jnp.float32)
        coef = jnp.where((degrees >= wave)[:, None], coef, 0.0).astype(jnp.bfloat16)
        mixed = jnp.dot(coef, weight, preferred_element_type=jnp.float32).astype(jnp.bfloat16)
        back = jnp.dot(table.T, mixed, preferred_element_type=jnp.float32) * lat_scale
        return back.astype(jnp.bfloat16)
    back = lax.map(one_slot, (legendre, spectrum, big, slot_wave))
    back = back.reshape(SLOTS, NLAT, 2, C)
    filtered = jnp.einsum('karc,rkn->anc', back.astype(jnp.float32), inverse.astype(jnp.float32)) * inv_root
    return (normed.astype(jnp.float32) + filtered).astype(jnp.bfloat16)
```

```python
import functools
import math

import jax
import jax.numpy as jnp
from jax import lax
from jax.experimental import pallas as pl
from jax.experimental.pallas import tpu as pltpu
from jax.sharding import PartitionSpec as P

MESH = pl.DeviceIdType.MESH


def exchange_kernel(count, each, x_ref, o_ref, send_sem, recv_sem, local_sem):
    me = lax.axis_index("lat")
    barrier = pltpu.get_barrier_semaphore()

    def greet(k, carry):
        pl.semaphore_signal(
            barrier, inc=1, device_id={"lat": lax.rem(me + k, count)}, device_id_type=MESH
        )
        return carry

    lax.fori_loop(1, count, greet, 0)
    pl.semaphore_wait(barrier, count - 1)
    own = pltpu.make_async_copy(x_ref.at[me] if each else x_ref, o_ref.at[me], local_sem)
    own.start()

    def send(k, carry):
        for step in (k, count - k):
            there = lax.rem(me + step, count)
            pltpu.make_async_remote_copy(
                src_ref=x_ref.at[there] if each else x_ref,
                dst_ref=o_ref.at[me],
                send_sem=send_sem,
                recv_sem=recv_sem,
                device_id={"lat": there},
                device_id_type=MESH,
            ).start()
        return carry

    lax.fori_loop(1, count // 2, send, 0)
    there = lax.rem(me + count // 2, count)
    pltpu.make_async_remote_copy(
        src_ref=x_ref.at[there] if each else x_ref,
        dst_ref=o_ref.at[me],
        send_sem=send_sem,
        recv_sem=recv_sem,
        device_id={"lat": there},
        device_id_type=MESH,
    ).start()
    own.wait()
    others = o_ref.at[pl.ds(0, count - 1)]
    pltpu.make_async_copy(others, others, send_sem).wait()
    pltpu.make_async_copy(others, others, recv_sem).wait()


def exchange(x, each, name, ident):
    count = lax.axis_size("lat")
    block = x.shape[1:] if each else x.shape
    return pl.pallas_call(
        functools.partial(exchange_kernel, count, each),
        out_shape=jax.ShapeDtypeStruct((count, *block), x.dtype),
        in_specs=[pl.BlockSpec(memory_space=pltpu.VMEM)],
        out_specs=pl.BlockSpec(memory_space=pltpu.VMEM),
        scratch_shapes=[pltpu.SemaphoreType.DMA] * 3,
        compiler_params=pltpu.CompilerParams(collective_id=ident, has_side_effects=True),
        name=name,
    )(x)


def phase_tables(waves, width):
    points = jnp.arange(width, dtype=jnp.int32)
    phase = (waves[:, None] * points[None, :] % width).astype(jnp.float32) * (2.0 * math.pi / width)
    return (jnp.cos(phase), jnp.sin(phase))


def block_weight(mixing):
    real_part = mixing[:, 0]
    imag_part = mixing[:, 1]
    upper = jnp.concatenate([real_part, imag_part], axis=2)
    lower = jnp.concatenate([-imag_part, real_part], axis=2)
    return jnp.concatenate([upper, lower], axis=1)


def per_device(field, gain, slot_wave, legendre, mixing):
    lat_count = lax.axis_size("lat")
    lat_dev, width, chans = field.shape
    slot_dev, degs, nlat = legendre.shape
    count = float(lat_dev * lat_count * width)
    values = field.astype(jnp.float32)
    local = jnp.stack([jnp.sum(values, axis=(0, 1)), jnp.sum(values * values, axis=(0, 1))])
    total, squares = jnp.sum(exchange(local, False, "sums", 0), axis=0)
    mean = total / count
    var = squares / count - mean * mean
    normed = ((values - mean) * (gain / jnp.sqrt(var + 1e-05))).astype(jnp.bfloat16)
    cosine, sine = phase_tables(slot_wave, width)
    table = jnp.stack([cosine, -sine], axis=1).astype(jnp.bfloat16)
    weight_m = jnp.where(slot_wave == 0, 1.0, 2.0).astype(jnp.bfloat16)[:, None, None]
    inv_root = 1.0 / math.sqrt(width)
    spectrum = (
        jnp.einsum("krn,anc->krac", table, normed, preferred_element_type=jnp.float32) * inv_root
    )
    spectrum = spectrum.astype(jnp.bfloat16).reshape(lat_count, -1, chans)
    arrived = exchange(spectrum, True, "there", 1)
    arrived = arrived.reshape(lat_count, slot_dev, 2, lat_dev, chans)
    arrived = arrived.transpose(1, 0, 3, 2, 4).reshape(slot_dev, nlat, 2 * chans)
    mine = lax.dynamic_slice_in_dim(slot_wave, lax.axis_index("lat") * slot_dev, slot_dev, 0)
    big = block_weight(mixing)
    lat_scale = math.sqrt(nlat / degs)
    degrees = jnp.arange(degs, dtype=jnp.int32)
    coef = jnp.einsum("jlt,jtc->jlc", legendre, arrived, preferred_element_type=jnp.float32)
    coef = jnp.where((degrees[None, :] >= mine[:, None])[:, :, None], coef, 0.0).astype(
        jnp.bfloat16
    )
    mixed = jnp.einsum("jlc,jcd->jld", coef, big, preferred_element_type=jnp.float32).astype(
        jnp.bfloat16
    )
    back = (
        jnp.einsum("jlt,jld->jtd", legendre, mixed, preferred_element_type=jnp.float32) * lat_scale
    )
    back = back.astype(jnp.bfloat16).reshape(slot_dev, lat_count, lat_dev, 2, chans)
    back = back.transpose(1, 0, 3, 2, 4).reshape(lat_count, -1, chans)
    returned = exchange(back, True, "home", 2)
    returned = returned.reshape(slot_dev * lat_count, 2, lat_dev, chans)
    filtered = (
        jnp.einsum(
            "krac,krn->anc", returned * weight_m[..., None], table, preferred_element_type=jnp.float32
        )
        * inv_root
    )
    return (normed.astype(jnp.float32) + filtered).astype(jnp.bfloat16)


def solution(mesh):
    return jax.shard_map(
        per_device,
        mesh=mesh,
        in_specs=(
            P(("member", "lat"), None, None),
            P(),
            P(),
            P("lat", None, None),
            P("lat", None, None, None),
        ),
        out_specs=P(("member", "lat"), None, None),
        check_vma=False,
    )
```

```python
import functools
import math

import jax
import jax.numpy as jnp
import numpy as np
from jax import lax
from jax.experimental import pallas as pl
from jax.experimental.pallas import tpu as pltpu
from jax.sharding import PartitionSpec as P

MESH = pl.DeviceIdType.MESH
F32 = jnp.float32
BF16 = jnp.bfloat16
HALVES = 2
PER_CHUNK = 2
GROUP = HALVES * PER_CHUNK * 2


def dot(a, b):
    return jnp.dot(a, b, preferred_element_type=F32)


def dot_tn(a, b):
    return lax.dot_general(a, b, (((0,), (0,)), ((), ())), preferred_element_type=F32)


def dot_nt(a, b):
    return lax.dot_general(a, b, (((1,), (1,)), ((), ())), preferred_element_type=F32)


def one_hot(target, rows):
    wide = jnp.broadcast_to(target, (rows, target.shape[1]))
    at = lax.broadcasted_iota(jnp.int32, wide.shape, 0)
    return jnp.where(at == wide, 1.0, 0.0).astype(BF16)


def layer_kernel(
    count,
    total_count,
    wave_ref,
    rowsum_ref,
    index_ref,
    lat_old_ref,
    lat_new_ref,
    gather_ref,
    scatter_ref,
    gain_ref,
    field_hbm,
    cos_hbm,
    legendre_hbm,
    mixing_hbm,
    out_hbm,
    field_v,
    cos_v,
    legendre_v,
    mixing_v,
    table_v,
    table_t_v,
    out_one,
    in_one,
    out_two,
    in_two,
    leg_v,
    leg_t_v,
    big_v,
    spec_v,
    z_v,
    masked_v,
    acc_v,
    mine_v,
    stats_v,
    shift_v,
    scale_v,
    send_sem,
    stat_sem,
    recv_one,
    recv_two,
    load_sem,
    store_sem,
):
    me = lax.axis_index("lat")
    lat_dev, width, chans = field_v.shape
    slots, degs, nlat = legendre_v.shape
    thirds = lat_dev // HALVES
    chunks = slots // PER_CHUNK
    rows = count * GROUP
    fold = HALVES * count
    inv_root = 1.0 / math.sqrt(width)
    lat_scale = math.sqrt(nlat / degs)

    barrier = pltpu.get_barrier_semaphore()

    def greet(k, carry):
        pl.semaphore_signal(
            barrier, inc=1, device_id={"lat": lax.rem(me + k, count)}, device_id_type=MESH
        )
        return carry

    lax.fori_loop(1, count, greet, 0)

    loads = [
        pltpu.make_async_copy(src, dst, load_sem.at[i])
        for i, (src, dst) in enumerate(
            (
                (field_hbm, field_v),
                (cos_hbm, cos_v),
                (legendre_hbm, legendre_v),
                (mixing_hbm, mixing_v),
            )
        )
    ]
    for load in loads:
        load.start()
    loads[0].wait()

    part = width // 10
    local_count = float(lat_dev * width)

    def add_rows(i, total):
        block = field_v[i // 10, pl.ds(pl.multiple_of((i % 10) * part, 16), part), :]
        return total + jnp.sum(block.astype(F32), axis=0, keepdims=True)

    mean_here = lax.fori_loop(0, lat_dev * 10, add_rows, jnp.zeros((1, chans), F32)) / local_count

    def add_squares(i, total):
        block = field_v[i // 10, pl.ds(pl.multiple_of((i % 10) * part, 16), part), :]
        off = block.astype(F32) - mean_here
        return total + jnp.sum(off * off, axis=0, keepdims=True)

    squares_here = lax.fori_loop(0, lat_dev * 10, add_squares, jnp.zeros((1, chans), F32))
    mine_v[0:1, :] = mean_here
    mine_v[1:2, :] = squares_here
    stats_v[me] = mine_v[...]

    loads[1].wait()

    def build_table(k, carry):
        table_v[k] = dot_tn(one_hot(index_ref[k], cos_v.shape[0]), cos_v[...]).astype(BF16)
        return carry

    row_half = lax.broadcasted_iota(jnp.int32, (rows, chans), 0) // (GROUP // HALVES) % HALVES

    def transform(k):
        sums = dot(table_v[k], jnp.ones((width, 128), BF16))[:, :1]

        def third(t, carry):
            low = dot(table_v[k], field_v[t])
            high = dot(table_v[k], field_v[thirds + t])
            both = (jnp.where(row_half == 0, low, high) - sums * mean_here) * inv_root
            out_one[
                pl.ds(k * count, count), :, pl.ds(pl.multiple_of(t * chans, 128), chans)
            ] = both.reshape(count, GROUP, chans).astype(BF16)
            return carry

        lax.fori_loop(0, thirds, third, 0)
        in_one[k * count + me] = out_one[k * count + me]

    def send_chunk(k, src, dst, recv):
        def send(there):
            pltpu.make_async_remote_copy(
                src_ref=src.at[k * count + there],
                dst_ref=dst.at[k * count + me],
                send_sem=send_sem,
                recv_sem=recv.at[k],
                device_id={"lat": there},
                device_id_type=MESH,
            ).start()

        def both(i, carry):
            send(lax.rem(me + i, count))
            send(lax.rem(me + count - i, count))
            return carry

        lax.fori_loop(1, count // 2, both, 0)
        send(lax.rem(me + count // 2, count))

    def wait_chunk(k, dst, recv):
        others = dst.at[pl.ds(k * count, count - 1)]
        pltpu.make_async_copy(others, others, recv.at[k]).wait()

    build_table(0, 0)
    transform(0)
    pl.semaphore_wait(barrier, count - 1)

    def send_stats(i, carry):
        there = lax.rem(me + i, count)
        pltpu.make_async_remote_copy(
            src_ref=mine_v,
            dst_ref=stats_v.at[me],
            send_sem=stat_sem.at[0],
            recv_sem=stat_sem.at[1],
            device_id={"lat": there},
            device_id_type=MESH,
        ).start()
        return carry

    lax.fori_loop(1, count, send_stats, 0)
    send_chunk(0, out_one, in_one, recv_one)

    def rest(k, carry):
        build_table(k, 0)
        transform(k)
        send_chunk(k, out_one, in_one, recv_one)
        return carry

    lax.fori_loop(1, chunks, rest, 0)

    loads[2].wait()
    loads[3].wait()

    def prepare(s, carry):
        leg_v[s] = dot(legendre_v[s], one_hot(lat_old_ref[...], nlat)).astype(BF16)
        leg_t_v[s] = dot_nt(one_hot(lat_new_ref[...], nlat), legendre_v[s]).astype(BF16)
        real = mixing_v[s, 0]
        imag = mixing_v[s, 1]
        big_v[s, :chans, :chans] = real
        big_v[s, :chans, chans:] = imag
        big_v[s, chans:, :chans] = -imag
        big_v[s, chans:, chans:] = real
        return carry

    lax.fori_loop(0, slots, prepare, 0)

    waves = cos_v.shape[0] // 2
    table_row = lax.broadcasted_iota(jnp.int32, (2 * waves, rows), 0)
    weight = jnp.where((table_row == 0) | (table_row == waves), 1.0, 2.0)

    def build_table_t(k, carry):
        chosen = (one_hot(index_ref[k], 2 * waves).astype(F32) * weight).astype(BF16)
        table_t_v[k] = dot_tn(cos_v[...], chosen).astype(BF16)
        return carry

    lax.fori_loop(0, chunks, build_table_t, 0)

    pltpu.make_async_copy(
        stats_v.at[pl.ds(0, count - 1)], stats_v.at[pl.ds(0, count - 1)], stat_sem.at[1]
    ).wait()
    means = stats_v[:, 0, :]
    mean = jnp.sum(means, axis=0, keepdims=True) / float(count)
    apart = means - mean
    var = (
        jnp.sum(stats_v[:, 1, :], axis=0, keepdims=True)
        + local_count * jnp.sum(apart * apart, axis=0, keepdims=True)
    ) / total_count
    scale = gain_ref[...] / jnp.sqrt(var + 1e-05)
    scale_v[0:1, :] = mean
    scale_v[1:2, :] = scale
    for h in range(HALVES):
        shift_v[h * count : (h + 1) * count, :] = apart * scale * inv_root

    def middle(k, carry):
        wait_chunk(k, in_one, recv_one)
        arrived = in_one[pl.ds(k * count, count)].reshape(rows, thirds * chans)
        ordered = dot(one_hot(gather_ref[...], rows), arrived)
        for q in range(PER_CHUNK * 2):
            j, r = q // 2, q % 2
            extra = shift_v[...] * rowsum_ref[k * PER_CHUNK + j, r]
            for t in range(thirds):
                block = ordered[q * fold : (q + 1) * fold, t * chans : (t + 1) * chans]
                spec_v[j, t * fold : (t + 1) * fold, r * chans : (r + 1) * chans] = (
                    block * scale_v[1:2, :] + extra
                ).astype(BF16)
        for j in range(PER_CHUNK):
            s = k * PER_CHUNK + j
            coef = dot(leg_v[s], spec_v[j])
            degree = lax.broadcasted_iota(jnp.int32, coef.shape, 0)
            coef = jnp.where(degree >= wave_ref[s], coef, 0.0).astype(BF16)
            mixed = dot(coef, big_v[s]).astype(BF16)
            back = (dot(leg_t_v[s], mixed) * lat_scale).astype(BF16)
            for r in range(2):
                q = 2 * j + r
                for t in range(thirds):
                    z_v[q * fold : (q + 1) * fold, t * chans : (t + 1) * chans] = back[
                        t * fold : (t + 1) * fold, r * chans : (r + 1) * chans
                    ]
        home = dot(one_hot(scatter_ref[...], rows), z_v[...])
        out_two[pl.ds(k * count, count)] = home.reshape(count, GROUP, thirds * chans).astype(BF16)
        in_two[k * count + me] = out_two[k * count + me]
        send_chunk(k, out_two, in_two, recv_two)
        return carry

    lax.fori_loop(0, chunks, middle, 0)

    blocks = 10
    lane_half = (
        lax.broadcasted_iota(jnp.int32, (rows, thirds * chans), 0) // (GROUP // HALVES) % HALVES
    )

    def take(k):
        wait_chunk(k, in_two, recv_two)
        returned = in_two[pl.ds(k * count, count)].reshape(rows, thirds * chans).astype(F32)
        for h in range(HALVES):
            masked_v[h] = jnp.where(lane_half == h, returned, 0.0).astype(BF16)

    take(0)

    def first_block(b, carry):
        at = pl.ds(pl.multiple_of(b * part, 16), part)
        for h in range(HALVES):
            acc_v[h, at, :] = dot(table_t_v[0, at, :], masked_v[h])
        return carry

    lax.fori_loop(0, blocks, first_block, 0)

    def inner(k, carry):
        take(k)

        def block(b, carry):
            at = pl.ds(pl.multiple_of(b * part, 16), part)
            for h in range(HALVES):
                acc_v[h, at, :] += dot(table_t_v[k, at, :], masked_v[h])
            return carry

        return lax.fori_loop(0, blocks, block, carry)

    lax.fori_loop(1, chunks - 1, inner, 0)
    take(chunks - 1)

    def last_block(b, carry):
        at = pl.ds(pl.multiple_of(b * part, 16), part)
        for h in range(HALVES):
            filtered = (acc_v[h, at, :] + dot(table_t_v[chunks - 1, at, :], masked_v[h])) * inv_root
            for t in range(thirds):
                a = h * thirds + t
                normed = (
                    (field_v[a, at, :].astype(F32) - scale_v[0:1, :]) * scale_v[1:2, :]
                ).astype(BF16)
                field_v[a, at, :] = (
                    normed.astype(F32) + filtered[:, t * chans : (t + 1) * chans]
                ).astype(BF16)
        pltpu.make_async_copy(field_v.at[:, at, :], out_hbm.at[:, at, :], store_sem).start()
        return carry

    lax.fori_loop(0, blocks, last_block, 0)
    pltpu.make_async_copy(field_v, out_hbm, store_sem).wait()
    pltpu.make_async_copy(
        stats_v.at[pl.ds(0, count - 1)], stats_v.at[pl.ds(0, count - 1)], stat_sem.at[0]
    ).wait()

    for k in range(2 * chunks):
        sent = in_one.at[pl.ds(0, count - 1)]
        pltpu.make_async_copy(sent, sent, send_sem).wait()


def cosine_rows(waves, width):
    points = np.arange(width, dtype=np.int64)[None, :] * np.arange(waves, dtype=np.int64)[:, None]
    phase = (points % width).astype(np.float32) * np.float32(2.0 * math.pi / width)
    return np.concatenate([np.cos(phase), -np.sin(phase)]).astype(jnp.bfloat16)


def per_device(field, gain, slot_wave, legendre, mixing):
    count = lax.axis_size("lat")
    lat_dev, width, chans = field.shape
    slots, degs, nlat = legendre.shape
    thirds = lat_dev // HALVES
    chunks = slots // PER_CHUNK
    rows = count * GROUP
    fold = HALVES * count
    wide = thirds * chans

    cosines = cosine_rows(degs, width)
    waves = slot_wave.reshape(count, chunks, 1, PER_CHUNK, 1)
    index = waves + degs * jnp.arange(2, dtype=jnp.int32)
    index = jnp.where(waves < degs, index, -1)
    index = jnp.broadcast_to(index, (count, chunks, HALVES, PER_CHUNK, 2))
    index = index.transpose(1, 0, 2, 3, 4).reshape(chunks, 1, rows)
    mine = lax.dynamic_slice_in_dim(slot_wave, lax.axis_index("lat") * slots, slots, 0)
    sums = np.sum(cosines.astype(np.float64), axis=1).astype(np.float32).reshape(2, degs)
    picked = mine[:, None] == jnp.arange(degs, dtype=jnp.int32)[None, :]
    rowsum = jnp.sum(jnp.where(picked[:, None, :], sums[None], 0.0), axis=2)

    d, h, t = np.meshgrid(np.arange(count), np.arange(HALVES), np.arange(thirds), indexing="ij")
    old = (d * lat_dev + h * thirds + t).reshape(-1)
    new = (t * fold + h * count + d).reshape(-1)
    lat_old = np.zeros((1, nlat), np.int32)
    lat_old[0, new] = old
    lat_new = np.zeros((1, nlat), np.int32)
    lat_new[0, old] = new
    d, h, q = np.meshgrid(
        np.arange(count), np.arange(HALVES), np.arange(2 * PER_CHUNK), indexing="ij"
    )
    came = (d * GROUP + h * 2 * PER_CHUNK + q).reshape(-1)
    goes = (q * fold + h * count + d).reshape(-1)
    gather = np.zeros((1, rows), np.int32)
    gather[0, came] = goes
    scatter = np.zeros((1, rows), np.int32)
    scatter[0, goes] = came

    smem = pl.BlockSpec(memory_space=pltpu.SMEM)
    vmem = pl.BlockSpec(memory_space=pltpu.VMEM)
    hbm = pl.BlockSpec(memory_space=pl.ANY)
    parcels = (chunks * count, GROUP, wide)
    return pl.pallas_call(
        functools.partial(layer_kernel, count, float(lat_dev * count * width)),
        out_shape=jax.ShapeDtypeStruct(field.shape, field.dtype),
        in_specs=[smem] * 2 + [vmem] * 6 + [hbm] * 4,
        out_specs=hbm,
        scratch_shapes=[
            pltpu.VMEM(field.shape, BF16),
            pltpu.VMEM((2 * degs, width), BF16),
            pltpu.VMEM(legendre.shape, BF16),
            pltpu.VMEM(mixing.shape, BF16),
            pltpu.VMEM((chunks, rows, width), BF16),
            pltpu.VMEM((chunks, width, rows), BF16),
            pltpu.VMEM(parcels, BF16),
            pltpu.VMEM(parcels, BF16),
            pltpu.VMEM(parcels, BF16),
            pltpu.VMEM(parcels, BF16),
            pltpu.VMEM((slots, degs, nlat), BF16),
            pltpu.VMEM((slots, nlat, degs), BF16),
            pltpu.VMEM((slots, 2 * chans, 2 * chans), BF16),
            pltpu.VMEM((PER_CHUNK, nlat, 2 * chans), BF16),
            pltpu.VMEM((rows, wide), BF16),
            pltpu.VMEM((HALVES, rows, wide), BF16),
            pltpu.VMEM((HALVES, width, wide), F32),
            pltpu.VMEM((2, chans), F32),
            pltpu.VMEM((count, 2, chans), F32),
            pltpu.VMEM((fold, chans), F32),
            pltpu.VMEM((2, chans), F32),
            pltpu.SemaphoreType.DMA,
            pltpu.SemaphoreType.DMA((2,)),
            pltpu.SemaphoreType.DMA((chunks,)),
            pltpu.SemaphoreType.DMA((chunks,)),
            pltpu.SemaphoreType.DMA((4,)),
            pltpu.SemaphoreType.DMA,
        ],
        compiler_params=pltpu.CompilerParams(
            collective_id=0, has_side_effects=True, vmem_limit_bytes=66_000_000
        ),
        name="layer",
    )(
        mine,
        rowsum,
        index,
        jnp.asarray(lat_old),
        jnp.asarray(lat_new),
        jnp.asarray(gather),
        jnp.asarray(scatter),
        gain[None],
        field,
        jnp.asarray(cosines),
        legendre,
        mixing,
    )


def solution(mesh):
    return jax.shard_map(
        per_device,
        mesh=mesh,
        in_specs=(
            P(("member", "lat"), None, None),
            P(),
            P(),
            P("lat", None, None),
            P("lat", None, None, None),
        ),
        out_specs=P(("member", "lat"), None, None),
        check_vma=False,
    )
```

```python
import functools
import math

import jax
import jax.numpy as jnp
import numpy as np
from jax import lax
from jax.experimental import pallas as pl
from jax.experimental.pallas import tpu as pltpu
from jax.sharding import PartitionSpec as P

MESH = pl.DeviceIdType.MESH
F32 = jnp.float32
BF16 = jnp.bfloat16
HALVES = 2
PER_CHUNK = 2
GROUP = HALVES * PER_CHUNK * 2


def dot(a, b):
    return jnp.dot(a, b, preferred_element_type=F32)


def dot_tn(a, b):
    return lax.dot_general(a, b, (((0,), (0,)), ((), ())), preferred_element_type=F32)


def dot_nt(a, b):
    return lax.dot_general(a, b, (((1,), (1,)), ((), ())), preferred_element_type=F32)


def one_hot(target, rows):
    wide = jnp.broadcast_to(target, (rows, target.shape[1]))
    at = lax.broadcasted_iota(jnp.int32, wide.shape, 0)
    return jnp.where(at == wide, 1.0, 0.0).astype(BF16)


def layer_kernel(
    count,
    total_count,
    wave_ref,
    rowsum_ref,
    wave_row_ref,
    slot_ref,
    lat_old_ref,
    lat_new_ref,
    gather_ref,
    scatter_ref,
    gain_ref,
    field_hbm,
    cos_hbm,
    legendre_hbm,
    mixing_hbm,
    out_hbm,
    field_v,
    cos_v,
    legendre_v,
    mixing_v,
    table_v,
    table_t_v,
    out_one,
    in_one,
    out_two,
    in_two,
    leg_v,
    leg_t_v,
    big_v,
    spec_v,
    z_v,
    masked_v,
    acc_v,
    chosen_v,
    mine_v,
    other_v,
    half_v,
    halves_v,
    total_v,
    rest_v,
    scale_v,
    send_sem,
    stat_sem,
    recv_one,
    recv_two,
    load_sem,
    store_sem,
):
    me = lax.axis_index("lat")
    lat_dev, width, chans = field_v.shape
    slots, degs, nlat = legendre_v.shape
    thirds = lat_dev // HALVES
    chunks = slots // PER_CHUNK
    rows = count * GROUP
    fold = HALVES * count
    degs_kept = cos_v.shape[0] // 2
    core = lax.rem(me, 2)
    partner = me + 1 - 2 * core
    inv_root = 1.0 / math.sqrt(width)
    lat_scale = math.sqrt(nlat / degs)

    barrier = pltpu.get_barrier_semaphore()

    def greet(k, carry):
        pl.semaphore_signal(
            barrier, inc=1, device_id={"lat": lax.rem(me + k, count)}, device_id_type=MESH
        )
        return carry

    lax.fori_loop(1, count, greet, 0)

    loads = [
        pltpu.make_async_copy(src, dst, load_sem.at[i])
        for i, (src, dst) in enumerate(
            (
                (field_hbm, field_v),
                (cos_hbm, cos_v),
                (legendre_hbm, legendre_v),
                (mixing_hbm, mixing_v),
            )
        )
    ]
    for load in loads:
        load.start()
    loads[0].wait()

    part = width // 10
    local_count = float(lat_dev * width)

    def add_rows(i, total):
        block = field_v[i // 10, pl.ds(pl.multiple_of((i % 10) * part, 16), part), :]
        return total + jnp.sum(block.astype(F32), axis=0, keepdims=True)

    mean_here = lax.fori_loop(0, lat_dev * 10, add_rows, jnp.zeros((1, chans), F32)) / local_count

    def add_squares(i, total):
        block = field_v[i // 10, pl.ds(pl.multiple_of((i % 10) * part, 16), part), :]
        off = block.astype(F32) - mean_here
        return total + jnp.sum(off * off, axis=0, keepdims=True)

    squares_here = lax.fori_loop(0, lat_dev * 10, add_squares, jnp.zeros((1, chans), F32))
    mine_v[0:1, :] = mean_here
    mine_v[1:2, :] = squares_here

    loads[1].wait()
    wave_of_slot = one_hot(wave_row_ref[...], degs_kept)

    def build_table(k):
        for r in range(2):
            row_slot = one_hot(slot_ref[k, r], wave_row_ref.shape[1])
            chosen_v[k, r * degs_kept : (r + 1) * degs_kept, :] = dot(wave_of_slot, row_slot).astype(
                BF16
            )
        table_v[k] = dot_tn(chosen_v[k], cos_v[...]).astype(BF16)

    row_half = lax.broadcasted_iota(jnp.int32, (rows, chans), 0) // (GROUP // HALVES) % HALVES

    def transform(k, pivot=None):
        offset = 0.0
        if pivot is not None:
            offset = dot(table_v[k], jnp.ones((width, 128), BF16))[:, :1] * pivot

        def third(t, carry):
            low = dot(table_v[k], field_v[t])
            high = dot(table_v[k], field_v[thirds + t])
            both = (jnp.where(row_half == 0, low, high) - offset) * inv_root
            out_one[
                pl.ds(k * count, count), :, pl.ds(pl.multiple_of(t * chans, 128), chans)
            ] = both.reshape(count, GROUP, chans).astype(BF16)
            return carry

        lax.fori_loop(0, thirds, third, 0)
        in_one[k * count + me] = out_one[k * count + me]

    def send_chunk(k, src, dst, recv):
        def send(there):
            pltpu.make_async_remote_copy(
                src_ref=src.at[k * count + there],
                dst_ref=dst.at[k * count + me],
                send_sem=send_sem,
                recv_sem=recv.at[k],
                device_id={"lat": there},
                device_id_type=MESH,
            ).start()

        def both(i, carry):
            step = jnp.where(lax.rem(i, 2) == 0, count // 2 - 1 - i // 2, (i + 1) // 2)
            send(lax.rem(me + step, count))
            send(lax.rem(me + count - step, count))
            return carry

        lax.fori_loop(0, count // 2 - 1, both, 0)
        send(lax.rem(me + count // 2, count))

    def wait_chunk(k, dst, recv):
        others = dst.at[pl.ds(k * count, count - 1)]
        pltpu.make_async_copy(others, others, recv.at[k]).wait()

    def tell(src, dst, sems, there):
        return pltpu.make_async_remote_copy(
            src_ref=src,
            dst_ref=dst,
            send_sem=stat_sem.at[sems],
            recv_sem=stat_sem.at[sems + 1],
            device_id={"lat": there},
            device_id_type=MESH,
        )

    build_table(1)
    transform(1)
    pl.semaphore_wait(barrier, count - 1)

    lanes = chans // 2
    pair = tell(mine_v, other_v, 0, partner)
    pair.start()
    pair.wait()
    gap = mine_v[0:1, :] - other_v[0:1, :]
    pair_mean = (mine_v[0:1, :] + other_v[0:1, :]) * 0.5
    pair_squares = mine_v[1:2, :] + other_v[1:2, :] + (0.5 * local_count) * gap * gap
    half_v[0:1, :] = jnp.where(core == 0, pair_mean[:, :lanes], pair_mean[:, lanes:])
    half_v[1:2, :] = jnp.where(core == 0, pair_squares[:, :lanes], pair_squares[:, lanes:])
    halves_v[me // 2] = half_v[...]

    def send_stats(i, carry):
        tell(half_v, halves_v.at[me // 2], 2, lax.rem(me + 2 * i, count)).start()
        return carry

    lax.fori_loop(1, count // 2, send_stats, 0)
    send_chunk(1, out_one, in_one, recv_one)

    def rest(k, carry):
        build_table(k)
        transform(k)
        send_chunk(k, out_one, in_one, recv_one)
        return carry

    lax.fori_loop(2, chunks, rest, 0)
    build_table(0)

    for sem in (2, 3):
        pltpu.make_async_copy(
            halves_v.at[pl.ds(0, count // 2 - 1)],
            halves_v.at[pl.ds(0, count // 2 - 1)],
            stat_sem.at[sem],
        ).wait()
    means = halves_v[:, 0, :]
    mean_half = jnp.sum(means, axis=0, keepdims=True) / float(count // 2)
    apart = means - mean_half
    total_v[0:1, :] = mean_half
    total_v[1:2, :] = (
        jnp.sum(halves_v[:, 1, :], axis=0, keepdims=True)
        + 2.0 * local_count * jnp.sum(apart * apart, axis=0, keepdims=True)
    ) / total_count
    share = tell(total_v, rest_v, 4, partner)
    share.start()
    share.wait()
    for i in range(2):
        scale_v[i : i + 1, :lanes] = jnp.where(
            core == 0, total_v[i : i + 1, :], rest_v[i : i + 1, :]
        )
        scale_v[i : i + 1, lanes:] = jnp.where(
            core == 0, rest_v[i : i + 1, :], total_v[i : i + 1, :]
        )
    mean = scale_v[0:1, :]
    scale_v[1:2, :] = gain_ref[...] / jnp.sqrt(scale_v[1:2, :] + 1e-05)
    transform(0, mean)
    send_chunk(0, out_one, in_one, recv_one)

    loads[2].wait()
    loads[3].wait()

    def prepare(s, carry):
        leg_v[s] = dot(legendre_v[s], one_hot(lat_old_ref[...], nlat)).astype(BF16)
        leg_t_v[s] = dot_nt(one_hot(lat_new_ref[...], nlat), legendre_v[s]).astype(BF16)
        real = mixing_v[s, 0]
        imag = mixing_v[s, 1]
        big_v[s, :chans, :chans] = real
        big_v[s, :chans, chans:] = imag
        big_v[s, chans:, :chans] = -imag
        big_v[s, chans:, chans:] = real
        return carry

    lax.fori_loop(0, slots, prepare, 0)

    table_row = lax.broadcasted_iota(jnp.int32, (2 * degs_kept, rows), 0)
    weight = jnp.where((table_row == 0) | (table_row == degs_kept), 1.0, 2.0)

    def build_table_t(k, carry):
        chosen = (chosen_v[k].astype(F32) * weight).astype(BF16)
        table_t_v[k] = dot_tn(cos_v[...], chosen).astype(BF16)
        return carry

    lax.fori_loop(0, chunks, build_table_t, 0)

    def middle(turn, carry):
        k = lax.rem(turn + 1, chunks)
        wait_chunk(k, in_one, recv_one)
        arrived = in_one[pl.ds(k * count, count)].reshape(rows, thirds * chans)
        ordered = dot(one_hot(gather_ref[...], rows), arrived)
        for q in range(PER_CHUNK * 2):
            j, r = q // 2, q % 2
            wave = jnp.minimum(wave_ref[me * slots + k * PER_CHUNK + j], degs_kept - 1)
            rowsum = jnp.where(k == 0, 0.0, rowsum_ref[r * degs_kept + wave])
            extra = scale_v[0:1, :] * scale_v[1:2, :] * (-inv_root * rowsum)
            for t in range(thirds):
                block = ordered[q * fold : (q + 1) * fold, t * chans : (t + 1) * chans]
                spec_v[j, t * fold : (t + 1) * fold, r * chans : (r + 1) * chans] = (
                    block * scale_v[1:2, :] + extra
                ).astype(BF16)
        for j in range(PER_CHUNK):
            s = k * PER_CHUNK + j
            coef = dot(leg_v[s], spec_v[j])
            degree = lax.broadcasted_iota(jnp.int32, coef.shape, 0)
            coef = jnp.where(degree >= wave_ref[me * slots + s], coef, 0.0).astype(BF16)
            mixed = dot(coef, big_v[s]).astype(BF16)
            back = (dot(leg_t_v[s], mixed) * lat_scale).astype(BF16)
            for r in range(2):
                q = 2 * j + r
                for t in range(thirds):
                    z_v[q * fold : (q + 1) * fold, t * chans : (t + 1) * chans] = back[
                        t * fold : (t + 1) * fold, r * chans : (r + 1) * chans
                    ]
        home = dot(one_hot(scatter_ref[...], rows), z_v[...])
        out_two[pl.ds(k * count, count)] = home.reshape(count, GROUP, thirds * chans).astype(BF16)
        in_two[k * count + me] = out_two[k * count + me]
        send_chunk(k, out_two, in_two, recv_two)
        return carry

    lax.fori_loop(0, chunks, middle, 0)

    blocks = 10
    lane_half = (
        lax.broadcasted_iota(jnp.int32, (rows, thirds * chans), 0) // (GROUP // HALVES) % HALVES
    )

    def take(k):
        wait_chunk(k, in_two, recv_two)
        returned = in_two[pl.ds(k * count, count)].reshape(rows, thirds * chans).astype(F32)
        for h in range(HALVES):
            masked_v[h] = jnp.where(lane_half == h, returned, 0.0).astype(BF16)

    take(1)

    def first_block(b, carry):
        at = pl.ds(pl.multiple_of(b * part, 16), part)
        for h in range(HALVES):
            acc_v[h, at, :] = dot(table_t_v[1, at, :], masked_v[h])
        return carry

    lax.fori_loop(0, blocks, first_block, 0)

    def inner(k, carry):
        take(k)

        def block(b, carry):
            at = pl.ds(pl.multiple_of(b * part, 16), part)
            for h in range(HALVES):
                acc_v[h, at, :] += dot(table_t_v[k, at, :], masked_v[h])
            return carry

        return lax.fori_loop(0, blocks, block, carry)

    lax.fori_loop(2, chunks, inner, 0)
    take(0)

    def last_block(b, carry):
        at = pl.ds(pl.multiple_of(b * part, 16), part)
        for h in range(HALVES):
            filtered = (acc_v[h, at, :] + dot(table_t_v[0, at, :], masked_v[h])) * inv_root
            for t in range(thirds):
                a = h * thirds + t
                normed = (
                    (field_v[a, at, :].astype(F32) - scale_v[0:1, :]) * scale_v[1:2, :]
                ).astype(BF16)
                field_v[a, at, :] = (
                    normed.astype(F32) + filtered[:, t * chans : (t + 1) * chans]
                ).astype(BF16)
        pltpu.make_async_copy(field_v.at[:, at, :], out_hbm.at[:, at, :], store_sem).start()
        return carry

    lax.fori_loop(0, blocks, last_block, 0)
    pltpu.make_async_copy(field_v, out_hbm, store_sem).wait()
    for k in range(2 * chunks):
        sent = in_one.at[pl.ds(0, count - 1)]
        pltpu.make_async_copy(sent, sent, send_sem).wait()


def cosine_rows(waves, width):
    points = np.arange(width, dtype=np.int64)[None, :] * np.arange(waves, dtype=np.int64)[:, None]
    phase = (points % width).astype(np.float32) * np.float32(2.0 * math.pi / width)
    return np.concatenate([np.cos(phase), -np.sin(phase)]).astype(jnp.bfloat16)


def per_device(field, gain, slot_wave, legendre, mixing):
    count = lax.axis_size("lat")
    lat_dev, width, chans = field.shape
    slots, degs, nlat = legendre.shape
    thirds = lat_dev // HALVES
    chunks = slots // PER_CHUNK
    rows = count * GROUP
    fold = HALVES * count
    wide = thirds * chans

    cosines = cosine_rows(degs, width)
    sums = np.sum(cosines.astype(np.float64), axis=1).astype(np.float32)
    k, r, d, _, j, part = np.meshgrid(
        np.arange(chunks),
        np.arange(2),
        np.arange(count),
        np.arange(HALVES),
        np.arange(PER_CHUNK),
        np.arange(2),
        indexing="ij",
    )
    slot = np.where(r == part, d * slots + k * PER_CHUNK + j, -1).astype(np.int32)
    slot = slot.reshape(chunks, 2, 1, rows)

    d, h, t = np.meshgrid(np.arange(count), np.arange(HALVES), np.arange(thirds), indexing="ij")
    old = (d * lat_dev + h * thirds + t).reshape(-1)
    new = (t * fold + h * count + d).reshape(-1)
    lat_old = np.zeros((1, nlat), np.int32)
    lat_old[0, new] = old
    lat_new = np.zeros((1, nlat), np.int32)
    lat_new[0, old] = new
    d, h, q = np.meshgrid(
        np.arange(count), np.arange(HALVES), np.arange(2 * PER_CHUNK), indexing="ij"
    )
    came = (d * GROUP + h * 2 * PER_CHUNK + q).reshape(-1)
    goes = (q * fold + h * count + d).reshape(-1)
    gather = np.zeros((1, rows), np.int32)
    gather[0, came] = goes
    scatter = np.zeros((1, rows), np.int32)
    scatter[0, goes] = came

    smem = pl.BlockSpec(memory_space=pltpu.SMEM)
    vmem = pl.BlockSpec(memory_space=pltpu.VMEM)
    hbm = pl.BlockSpec(memory_space=pl.ANY)
    parcels = (chunks * count, GROUP, wide)
    return pl.pallas_call(
        functools.partial(layer_kernel, count, float(lat_dev * count * width)),
        out_shape=jax.ShapeDtypeStruct(field.shape, field.dtype),
        in_specs=[smem] * 2 + [vmem] * 7 + [hbm] * 4,
        out_specs=hbm,
        scratch_shapes=[
            pltpu.VMEM(field.shape, BF16),
            pltpu.VMEM((2 * degs, width), BF16),
            pltpu.VMEM(legendre.shape, BF16),
            pltpu.VMEM(mixing.shape, BF16),
            pltpu.VMEM((chunks, rows, width), BF16),
            pltpu.VMEM((chunks, width, rows), BF16),
            pltpu.VMEM(parcels, BF16),
            pltpu.VMEM(parcels, BF16),
            pltpu.VMEM(parcels, BF16),
            pltpu.VMEM(parcels, BF16),
            pltpu.VMEM((slots, degs, nlat), BF16),
            pltpu.VMEM((slots, nlat, degs), BF16),
            pltpu.VMEM((slots, 2 * chans, 2 * chans), BF16),
            pltpu.VMEM((PER_CHUNK, nlat, 2 * chans), BF16),
            pltpu.VMEM((rows, wide), BF16),
            pltpu.VMEM((HALVES, rows, wide), BF16),
            pltpu.VMEM((HALVES, width, wide), F32),
            pltpu.VMEM((chunks, 2 * degs, rows), BF16),
            pltpu.VMEM((2, chans), F32),
            pltpu.VMEM((2, chans), F32),
            pltpu.VMEM((2, chans // 2), F32),
            pltpu.VMEM((count // 2, 2, chans // 2), F32),
            pltpu.VMEM((2, chans // 2), F32),
            pltpu.VMEM((2, chans // 2), F32),
            pltpu.VMEM((2, chans), F32),
            pltpu.SemaphoreType.DMA,
            pltpu.SemaphoreType.DMA((6,)),
            pltpu.SemaphoreType.DMA((chunks,)),
            pltpu.SemaphoreType.DMA((chunks,)),
            pltpu.SemaphoreType.DMA((4,)),
            pltpu.SemaphoreType.DMA,
        ],
        compiler_params=pltpu.CompilerParams(
            collective_id=0, has_side_effects=True, vmem_limit_bytes=66_000_000
        ),
        name="layer",
    )(
        slot_wave,
        jnp.asarray(sums),
        slot_wave[None],
        jnp.asarray(slot),
        jnp.asarray(lat_old),
        jnp.asarray(lat_new),
        jnp.asarray(gather),
        jnp.asarray(scatter),
        gain[None],
        field,
        jnp.asarray(cosines),
        legendre,
        mixing,
    )


def solution(mesh):
    return jax.shard_map(
        per_device,
        mesh=mesh,
        in_specs=(
            P(("member", "lat"), None, None),
            P(),
            P(),
            P("lat", None, None),
            P("lat", None, None, None),
        ),
        out_specs=P(("member", "lat"), None, None),
        check_vma=False,
    )
```

```python
import functools
import math

import jax
import jax.numpy as jnp
import numpy as np
from jax import lax
from jax.experimental import pallas as pl
from jax.experimental.pallas import tpu as pltpu
from jax.sharding import PartitionSpec as P

MESH = pl.DeviceIdType.MESH
F32 = jnp.float32
BF16 = jnp.bfloat16
HALVES = 2
PER_CHUNK = 2
GROUP = HALVES * PER_CHUNK * 2
HUB_LATS = 128
SIDES = (1, -1)


def dot(a, b):
    return jnp.dot(a, b, preferred_element_type=F32)


def dot_tn(a, b):
    return lax.dot_general(a, b, (((0,), (0,)), ((), ())), preferred_element_type=F32)


def dot_nt(a, b):
    return lax.dot_general(a, b, (((1,), (1,)), ((), ())), preferred_element_type=F32)


def one_hot(target, rows):
    wide = jnp.broadcast_to(target, (rows, target.shape[1]))
    at = lax.broadcasted_iota(jnp.int32, wide.shape, 0)
    return jnp.where(at == wide, 1.0, 0.0).astype(BF16)


def layer_kernel(
    count,
    total_count,
    wave_ref,
    rowsum_ref,
    wave_row_ref,
    slot_ref,
    lat_old_ref,
    lat_new_ref,
    gather_ref,
    scatter_ref,
    hub_chip_ref,
    hub_inner_ref,
    hub_lane_ref,
    hub_gather_ref,
    hub_scatter_ref,
    gain_ref,
    field_hbm,
    cos_hbm,
    legendre_hbm,
    mixing_hbm,
    out_hbm,
    field_v,
    cos_v,
    legendre_v,
    mixing_v,
    table_v,
    table_t_v,
    out_one,
    in_one,
    out_two,
    in_two,
    leg_v,
    leg_t_v,
    big_v,
    spec_v,
    z_v,
    masked_v,
    acc_v,
    chosen_v,
    hub_in,
    hub_out,
    leg_out,
    leg_in,
    part_out,
    part_in,
    mix_out,
    mix_in,
    coef_v,
    mixed_v,
    hub_spec_v,
    hub_z_v,
    mine_v,
    other_v,
    half_v,
    halves_v,
    total_v,
    rest_v,
    scale_v,
    send_sem,
    stat_sem,
    recv_one,
    recv_two,
    hub_sem,
    leg_sem,
    part_sem,
    mix_sem,
    load_sem,
    store_sem,
):
    me = lax.axis_index("lat")
    lat_dev, width, chans = field_v.shape
    slots, degs, nlat = legendre_v.shape
    thirds = lat_dev // HALVES
    chunks = slots // PER_CHUNK
    rows = count * GROUP
    fold = HALVES * count
    degs_kept = cos_v.shape[0] // 2
    core = lax.rem(me, 2)
    partner = me + 1 - 2 * core
    chip = me // 2
    chips = count // 2
    far = chips // 2
    served = hub_in.shape[1]
    reach = far - (served - 1) // 2
    packed = part_in.shape[1]
    hub_fold = hub_spec_v.shape[1] // thirds
    last = chunks - 1
    near = 2 * (2 * reach - 1)

    def device(at_chip, at_core):
        return 2 * lax.rem(at_chip + 2 * chips, chips) + at_core

    inv_root = 1.0 / math.sqrt(width)
    lat_scale = math.sqrt(nlat / degs)

    barrier = pltpu.get_barrier_semaphore()

    def greet(k, carry):
        pl.semaphore_signal(
            barrier, inc=1, device_id={"lat": lax.rem(me + k, count)}, device_id_type=MESH
        )
        return carry

    in_one[last * count : (last + 1) * count] = jnp.zeros((count, *in_one.shape[1:]), BF16)
    lax.fori_loop(1, count, greet, 0)

    loads = [
        pltpu.make_async_copy(src, dst, load_sem.at[i])
        for i, (src, dst) in enumerate(
            (
                (field_hbm, field_v),
                (cos_hbm, cos_v),
                (legendre_hbm, legendre_v),
                (mixing_hbm, mixing_v),
            )
        )
    ]
    for load in loads:
        load.start()
    loads[0].wait()

    part = width // 10
    local_count = float(lat_dev * width)

    def add_rows(i, total):
        block = field_v[i // 10, pl.ds(pl.multiple_of((i % 10) * part, 16), part), :]
        return total + jnp.sum(block.astype(F32), axis=0, keepdims=True)

    mean_here = lax.fori_loop(0, lat_dev * 10, add_rows, jnp.zeros((1, chans), F32)) / local_count

    def add_squares(i, total):
        block = field_v[i // 10, pl.ds(pl.multiple_of((i % 10) * part, 16), part), :]
        off = block.astype(F32) - mean_here
        return total + jnp.sum(off * off, axis=0, keepdims=True)

    squares_here = lax.fori_loop(0, lat_dev * 10, add_squares, jnp.zeros((1, chans), F32))
    mine_v[0:1, :] = mean_here
    mine_v[1:2, :] = squares_here

    loads[1].wait()
    wave_of_slot = one_hot(wave_row_ref[...], degs_kept)

    def build_table(k):
        for r in range(2):
            row_slot = one_hot(slot_ref[k, r], wave_row_ref.shape[1])
            chosen_v[k, r * degs_kept : (r + 1) * degs_kept, :] = dot(wave_of_slot, row_slot).astype(
                BF16
            )
        table_v[k] = dot_tn(chosen_v[k], cos_v[...]).astype(BF16)

    row_half = lax.broadcasted_iota(jnp.int32, (rows, chans), 0) // (GROUP // HALVES) % HALVES

    def transform(k):
        offset = dot(table_v[k], jnp.ones((width, 128), BF16))[:, :1] * scale_v[0:1, :]

        def third(t, carry):
            low = dot(table_v[k], field_v[t])
            high = dot(table_v[k], field_v[thirds + t])
            both = (jnp.where(row_half == 0, low, high) - offset) * inv_root
            out_one[
                pl.ds(k * count, count), :, pl.ds(pl.multiple_of(t * chans, 128), chans)
            ] = both.reshape(count, GROUP, chans).astype(BF16)
            return carry

        lax.fori_loop(0, thirds, third, 0)

    def parcel(src, dst, there, recv):
        pltpu.make_async_remote_copy(
            src_ref=src,
            dst_ref=dst,
            send_sem=send_sem,
            recv_sem=recv,
            device_id={"lat": there},
            device_id_type=MESH,
        ).start()

    def send_near(src, dst, recv):
        first = device(chip - (reach - 1), 0)

        def send(i, carry):
            step = lax.rem(2 * (reach - 1) + core + i, near)
            there = lax.rem(first + step, count)
            parcel(src.at[last * count + there], dst.at[last * count + me], there, recv.at[last])
            return carry

        lax.fori_loop(1, near, send, 0)

    def send_to_hubs():
        def block(owner):
            return out_one.at[last * count + owner]

        side_here = 1 - 2 * core
        for to in range(2):
            there = device(chip - side_here * (far - reach), to)
            parcel(
                block(device(chip + far, to)),
                hub_in.at[core, served - 1],
                there,
                hub_sem.at[core],
            )
        for i, side in enumerate(SIDES):

            def send(v, carry):
                e, to = v // 2, lax.rem(v, 2)
                parcel(
                    block(device(chip - side * (e + reach), to)),
                    hub_in.at[i, 2 * e + core],
                    device(chip - side * e, to),
                    hub_sem.at[i],
                )
                return carry

            lax.fori_loop(2, served - 1, send, 0)
            parcel(
                block(device(chip - side * reach, 1 - core)),
                hub_in.at[i, core],
                partner,
                hub_sem.at[i],
            )
            hub_in[i, core] = out_one[last * count + device(chip - side * reach, core)]

    def send_from_hub(i):
        side = SIDES[i]
        owner = device(chip - side * reach, core)
        dst = in_two.at[last * count + owner]

        def send(v, carry):
            there = device(chip + side * (v // 2), lax.rem(v, 2))
            parcel(hub_out.at[i, v], dst, there, recv_two.at[last])
            return carry

        lax.fori_loop(2, served - 1, send, 0)
        parcel(hub_out.at[i, 1 - core], dst, partner, recv_two.at[last])
        there = device(chip + side * (far - reach), i)
        parcel(hub_out.at[i, served - 1], dst, there, recv_two.at[last])
        in_two[last * count + owner] = hub_out[i, core]

    def to_side(src, dst, sems, i, toward):
        return pltpu.make_async_remote_copy(
            src_ref=src,
            dst_ref=dst.at[i],
            send_sem=sems.at[i],
            recv_sem=sems.at[2 + i],
            device_id={"lat": device(chip + toward * SIDES[i] * reach, core)},
            device_id_type=MESH,
        )

    def wave_at(owner, j):
        return wave_ref[owner * slots + last * PER_CHUNK + j]

    def pack(owner, j):
        low = degs - wave_at(owner, 0)
        begin = jnp.where(j == 0, 0, low)
        end = begin + degs - wave_at(owner, j)
        degree = lax.broadcasted_iota(jnp.int32, (degs, packed), 0)
        row = lax.broadcasted_iota(jnp.int32, (degs, packed), 1)
        hit = (degree - row == wave_at(owner, j) - begin) & (row >= begin) & (row < end)
        return jnp.where(hit, 1.0, 0.0).astype(BF16)

    def hub_legendre(i):
        return dot(leg_in[i], one_hot(hub_lane_ref[...], HUB_LATS)).astype(BF16)

    def of_slot(i, j, value):
        low = degs - wave_at(device(chip - SIDES[i] * reach, core), 0)
        row = lax.broadcasted_iota(jnp.int32, value.shape, 0)
        return jnp.where((row < low) == (j == 0), value, 0.0)

    def send_chunk(k, src, dst, recv):
        def send(there):
            pltpu.make_async_remote_copy(
                src_ref=src.at[k * count + there],
                dst_ref=dst.at[k * count + me],
                send_sem=send_sem,
                recv_sem=recv.at[k],
                device_id={"lat": there},
                device_id_type=MESH,
            ).start()

        def both(i, carry):
            step = jnp.where(lax.rem(i, 2) == 0, count // 2 - 1 - i // 2, (i + 1) // 2)
            send(lax.rem(me + step, count))
            send(lax.rem(me + count - step, count))
            return carry

        lax.fori_loop(0, count // 2 - 1, both, 0)
        send(lax.rem(me + count // 2, count))

    def wait_chunk(k, dst, recv, parcels):
        others = dst.at[pl.ds(k * count, parcels)]
        pltpu.make_async_copy(others, others, recv.at[k]).wait()

    def tell(src, dst, sems, there):
        return pltpu.make_async_remote_copy(
            src_ref=src,
            dst_ref=dst,
            send_sem=stat_sem.at[sems],
            recv_sem=stat_sem.at[sems + 1],
            device_id={"lat": there},
            device_id_type=MESH,
        )

    lanes = chans // 2
    def normalise(block, owner, k, j, r, keep):
        wave = jnp.minimum(wave_ref[owner * slots + k * PER_CHUNK + j], degs_kept - 1)
        rowsum = jnp.where(k == 0, 0.0, rowsum_ref[r * degs_kept + wave])
        extra = scale_v[0:1, :] * scale_v[1:2, :] * (-inv_root * rowsum)
        return (block * scale_v[1:2, :] + extra * keep).astype(BF16)

    def hub_forward():
        for sem in (2, 3):
            pltpu.make_async_copy(
                halves_v.at[pl.ds(0, count // 2 - 1)],
                halves_v.at[pl.ds(0, count // 2 - 1)],
                stat_sem.at[sem],
            ).wait()
        means = halves_v[:, 0, :]
        mean_half = jnp.sum(means, axis=0, keepdims=True) / float(count // 2)
        apart = means - mean_half
        total_v[0:1, :] = mean_half
        total_v[1:2, :] = (
            jnp.sum(halves_v[:, 1, :], axis=0, keepdims=True)
            + 2.0 * local_count * jnp.sum(apart * apart, axis=0, keepdims=True)
        ) / total_count
        share = tell(total_v, rest_v, 4, partner)
        share.start()
        share.wait()
        for i in range(2):
            scale_v[i : i + 1, :lanes] = jnp.where(
                core == 0, total_v[i : i + 1, :], rest_v[i : i + 1, :]
            )
            scale_v[i : i + 1, lanes:] = jnp.where(
                core == 0, rest_v[i : i + 1, :], total_v[i : i + 1, :]
            )
        scale_v[1:2, :] = gain_ref[...] / jnp.sqrt(scale_v[1:2, :] + 1e-05)

        for i in range(2):
            to_side(leg_out.at[i], leg_in, leg_sem, i, 1).wait()
            pltpu.make_async_copy(
                hub_in.at[i, pl.ds(0, served - 1)], hub_in.at[i, pl.ds(0, served - 1)], hub_sem.at[i]
            ).wait()
            owner = device(chip - SIDES[i] * reach, core)
            arrived = hub_in[i].reshape(served * GROUP, thirds * chans)
            ordered = dot(one_hot(hub_gather_ref[...], 2 * PER_CHUNK * hub_fold), arrived)
            for q in range(2 * PER_CHUNK):
                j, r = q // 2, q % 2
                for t in range(thirds):
                    block = ordered[q * hub_fold : (q + 1) * hub_fold, t * chans : (t + 1) * chans]
                    hub_spec_v[j, t * hub_fold : (t + 1) * hub_fold, r * chans : (r + 1) * chans] = (
                        normalise(block, owner, last, j, r, 1.0)
                    )
            leg = hub_legendre(i)
            total = of_slot(i, 0, dot(leg, hub_spec_v[0])) + of_slot(i, 1, dot(leg, hub_spec_v[1]))
            part_out[i] = total.astype(BF16)
            to_side(part_out.at[i], part_in, part_sem, i, -1).start()

    scale_v[...] = jnp.zeros_like(scale_v)
    acc_v[...] = jnp.zeros_like(acc_v)

    build_table(last)
    transform(last)
    loads[2].wait()
    for i, side in enumerate(SIDES):
        at_chip = lax.rem(chip + side * hub_chip_ref[...] + 2 * chips, chips)
        lats = one_hot(at_chip * (2 * lat_dev) + hub_inner_ref[i], nlat)
        rows_here = jnp.zeros((packed, HUB_LATS), F32)
        for j in range(PER_CHUNK):
            values = dot(legendre_v[last * PER_CHUNK + j], lats).astype(BF16)
            rows_here += dot_tn(pack(me, j), values)
        leg_out[i] = rows_here.astype(BF16)
    pl.semaphore_wait(barrier, count - 1)

    pair = tell(mine_v, other_v, 0, partner)
    pair.start()
    pair.wait()
    gap = mine_v[0:1, :] - other_v[0:1, :]
    pair_mean = (mine_v[0:1, :] + other_v[0:1, :]) * 0.5
    pair_squares = mine_v[1:2, :] + other_v[1:2, :] + (0.5 * local_count) * gap * gap
    half_v[0:1, :] = jnp.where(core == 0, pair_mean[:, :lanes], pair_mean[:, lanes:])
    half_v[1:2, :] = jnp.where(core == 0, pair_squares[:, :lanes], pair_squares[:, lanes:])
    halves_v[me // 2] = half_v[...]

    def send_stats(i, carry):
        tell(half_v, halves_v.at[me // 2], 2, lax.rem(me + 2 * i, count)).start()
        return carry

    lax.fori_loop(1, count // 2, send_stats, 0)
    for i in range(2):
        to_side(leg_out.at[i], leg_in, leg_sem, i, 1).start()
    send_to_hubs()
    send_near(out_one, in_one, recv_one)
    in_one[last * count + me] = out_one[last * count + me]

    def outward(turn, carry):
        k = last - turn
        build_table(k)
        pl.when(k == 0)(hub_forward)
        transform(k)
        send_chunk(k, out_one, in_one, recv_one)
        in_one[k * count + me] = out_one[k * count + me]
        return carry

    lax.fori_loop(1, chunks, outward, 0)

    loads[3].wait()

    def prepare(s, carry):
        leg_v[s] = dot(legendre_v[s], one_hot(lat_old_ref[...], nlat)).astype(BF16)
        leg_t_v[s] = dot_nt(one_hot(lat_new_ref[...], nlat), legendre_v[s]).astype(BF16)
        real = mixing_v[s, 0]
        imag = mixing_v[s, 1]
        big_v[s, :chans, :chans] = real
        big_v[s, :chans, chans:] = imag
        big_v[s, chans:, :chans] = -imag
        big_v[s, chans:, chans:] = real
        return carry

    lax.fori_loop(0, slots, prepare, 0)

    table_row = lax.broadcasted_iota(jnp.int32, (2 * degs_kept, rows), 0)
    weight = jnp.where((table_row == 0) | (table_row == degs_kept), 1.0, 2.0)

    def build_table_t(k, carry):
        chosen = (chosen_v[k].astype(F32) * weight).astype(BF16)
        table_t_v[k] = dot_tn(cos_v[...], chosen).astype(BF16)
        return carry

    lax.fori_loop(0, chunks, build_table_t, 0)

    place = lax.rem(lax.broadcasted_iota(jnp.int32, (fold, chans), 0), count) // 2
    apart_chips = jnp.abs(place - chip)
    close = jnp.minimum(apart_chips, chips - apart_chips) < reach

    def middle(turn, carry):
        k = last - turn

        @pl.when(k == last)
        def _():
            wait_chunk(last, in_one, recv_one, near - 1)
            for i in range(2):
                to_side(part_out.at[i], part_in, part_sem, i, -1).wait()

        @pl.when(k == 0)
        def _():
            for i in range(2):
                to_side(mix_out, mix_in, mix_sem, i, 1).wait()
                leg = hub_legendre(i)
                for j in range(PER_CHUNK):
                    rows_j = of_slot(i, j, mix_in[i].astype(F32)).astype(BF16)
                    back = (dot_tn(leg, rows_j) * lat_scale).astype(BF16)
                    for r in range(2):
                        q = 2 * j + r
                        for t in range(thirds):
                            hub_z_v[
                                q * hub_fold : (q + 1) * hub_fold, t * chans : (t + 1) * chans
                            ] = back[t * hub_fold : (t + 1) * hub_fold, r * chans : (r + 1) * chans]
                home = dot(one_hot(hub_scatter_ref[...], served * GROUP), hub_z_v[...])
                hub_out[i] = home.reshape(served, GROUP, thirds * chans).astype(BF16)
                send_from_hub(i)

        @pl.when(k != last)
        def _():
            wait_chunk(k, in_one, recv_one, count - 1)

        arrived = in_one[pl.ds(k * count, count)].reshape(rows, thirds * chans)
        ordered = dot(one_hot(gather_ref[...], rows), arrived)
        keep = jnp.where(close | (k != last), 1.0, 0.0)
        for q in range(PER_CHUNK * 2):
            j, r = q // 2, q % 2
            for t in range(thirds):
                block = ordered[q * fold : (q + 1) * fold, t * chans : (t + 1) * chans]
                spec_v[j, t * fold : (t + 1) * fold, r * chans : (r + 1) * chans] = normalise(
                    block, me, k, j, r, keep
                )

        def one_slot(j, carry):
            s = k * PER_CHUNK + j
            coef_v[...] = dot(leg_v[s], spec_v[j])

            @pl.when(k == last)
            def _():
                for i in range(2):
                    coef_v[...] += dot(pack(me, j), part_in[i])

            degree = lax.broadcasted_iota(jnp.int32, coef_v.shape, 0)
            coef = jnp.where(degree >= wave_ref[me * slots + s], coef_v[...], 0.0).astype(BF16)
            mixed_v[j] = dot(coef, big_v[s]).astype(BF16)
            back = (dot(leg_t_v[s], mixed_v[j]) * lat_scale).astype(BF16)
            for r in range(2):
                q = 2 * j + r
                for t in range(thirds):
                    z_v[
                        pl.ds(pl.multiple_of(q * fold, 16), fold), t * chans : (t + 1) * chans
                    ] = back[
                        t * fold : (t + 1) * fold, r * chans : (r + 1) * chans
                    ]
            return carry

        lax.fori_loop(0, PER_CHUNK, one_slot, 0)
        home = dot(one_hot(scatter_ref[...], rows), z_v[...])
        out_two[pl.ds(k * count, count)] = home.reshape(count, GROUP, thirds * chans).astype(BF16)
        in_two[k * count + me] = out_two[k * count + me]

        @pl.when(k == last)
        def _():
            mix_out[...] = (
                dot_tn(pack(me, 0), mixed_v[0]) + dot_tn(pack(me, 1), mixed_v[1])
            ).astype(BF16)
            for i in range(2):
                to_side(mix_out, mix_in, mix_sem, i, 1).start()
            send_near(out_two, in_two, recv_two)

        @pl.when(k != last)
        def _():
            send_chunk(k, out_two, in_two, recv_two)

        return carry

    lax.fori_loop(0, chunks, middle, 0)

    blocks = 10
    lane_half = (
        lax.broadcasted_iota(jnp.int32, (rows, thirds * chans), 0) // (GROUP // HALVES) % HALVES
    )

    def take(k):
        returned = in_two[pl.ds(k * count, count)].reshape(rows, thirds * chans).astype(F32)
        for h in range(HALVES):
            masked_v[h] = jnp.where(lane_half == h, returned, 0.0).astype(BF16)

    def inner(turn, carry):
        k = last - turn
        pl.when(k == last)(lambda: wait_chunk(last, in_two, recv_two, count - 3))
        pl.when(k != last)(lambda: wait_chunk(k, in_two, recv_two, count - 1))
        take(k)

        def block(i, carry):
            h = i // blocks
            at = pl.ds(pl.multiple_of(lax.rem(i, blocks) * part, 16), part)
            acc_v[h, at, :] += dot(table_t_v[k, at, :], masked_v[h])
            return carry

        return lax.fori_loop(0, HALVES * blocks, block, carry)

    lax.fori_loop(0, chunks - 1, inner, 0)
    wait_chunk(0, in_two, recv_two, count - 1)
    take(0)

    def last_block(i, carry):
        h = i // blocks
        at = pl.ds(pl.multiple_of(lax.rem(i, blocks) * part, 16), part)
        filtered = (acc_v[h, at, :] + dot(table_t_v[0, at, :], masked_v[h])) * inv_root
        for t in range(thirds):
            a = h * thirds + t
            normed = (
                (field_v[a, at, :].astype(F32) - scale_v[0:1, :]) * scale_v[1:2, :]
            ).astype(BF16)
            field_v[a, at, :] = (
                normed.astype(F32) + filtered[:, t * chans : (t + 1) * chans]
            ).astype(BF16)
        these = pl.ds(h * thirds, thirds)
        pltpu.make_async_copy(field_v.at[these, at, :], out_hbm.at[these, at, :], store_sem).start()
        return carry

    lax.fori_loop(0, HALVES * blocks, last_block, 0)
    pltpu.make_async_copy(field_v, out_hbm, store_sem).wait()
    for amount in [count - 1] * (2 * last) + [near - 1, 2 * (served - 1)] * 2:
        sent = in_one.at[pl.ds(0, amount)]
        pltpu.make_async_copy(sent, sent, send_sem).wait()


def cosine_rows(waves, width):
    points = np.arange(width, dtype=np.int64)[None, :] * np.arange(waves, dtype=np.int64)[:, None]
    phase = (points % width).astype(np.float32) * np.float32(2.0 * math.pi / width)
    return np.concatenate([np.cos(phase), -np.sin(phase)]).astype(jnp.bfloat16)


def per_device(field, gain, slot_wave, legendre, mixing):
    count = lax.axis_size("lat")
    lat_dev, width, chans = field.shape
    slots, degs, nlat = legendre.shape
    thirds = lat_dev // HALVES
    chunks = slots // PER_CHUNK
    rows = count * GROUP
    fold = HALVES * count
    wide = thirds * chans

    cosines = cosine_rows(degs, width)
    sums = np.sum(cosines.astype(np.float64), axis=1).astype(np.float32)
    k, r, d, _, j, part = np.meshgrid(
        np.arange(chunks),
        np.arange(2),
        np.arange(count),
        np.arange(HALVES),
        np.arange(PER_CHUNK),
        np.arange(2),
        indexing="ij",
    )
    slot = np.where(r == part, d * slots + k * PER_CHUNK + j, -1).astype(np.int32)
    slot = slot.reshape(chunks, 2, 1, rows)

    d, h, t = np.meshgrid(np.arange(count), np.arange(HALVES), np.arange(thirds), indexing="ij")
    old = (d * lat_dev + h * thirds + t).reshape(-1)
    new = (t * fold + h * count + d).reshape(-1)
    lat_old = np.zeros((1, nlat), np.int32)
    lat_old[0, new] = old
    lat_new = np.zeros((1, nlat), np.int32)
    lat_new[0, old] = new
    d, h, q = np.meshgrid(
        np.arange(count), np.arange(HALVES), np.arange(2 * PER_CHUNK), indexing="ij"
    )
    came = (d * GROUP + h * 2 * PER_CHUNK + q).reshape(-1)
    goes = (q * fold + h * count + d).reshape(-1)
    gather = np.zeros((1, rows), np.int32)
    gather[0, came] = goes
    scatter = np.zeros((1, rows), np.int32)
    scatter[0, goes] = came

    far = count // 4
    served = 2 * (far - 2) + 1
    while served * lat_dev > HUB_LATS:
        served -= 2
    reach = far - (served - 1) // 2
    hub_fold = HALVES * (-(-served // 8) * 8)
    packed = -(-(2 * degs - (4 * (chunks - 1) + 2) * count + 1) // 8) * 8
    t, h, p = np.meshgrid(
        np.arange(thirds), np.arange(HALVES), np.arange(served), indexing="ij"
    )
    lane = np.arange(t.size)
    hub_chip = np.zeros((1, HUB_LATS), np.int32)
    hub_chip[0, lane] = (reach + p // 2).reshape(-1)
    hub_inner = np.full((2, 1, HUB_LATS), -(2**20), np.int32)
    for i in range(2):
        at_core = np.where(p == served - 1, i, p % 2)
        hub_inner[i, 0, lane] = (at_core * lat_dev + h * thirds + t).reshape(-1)
    hub_lane = np.full((1, thirds * hub_fold), -1, np.int32)
    hub_lane[0, (t * hub_fold + h * (hub_fold // HALVES) + p).reshape(-1)] = lane
    p, h, q = np.meshgrid(
        np.arange(served), np.arange(HALVES), np.arange(2 * PER_CHUNK), indexing="ij"
    )
    came = (p * GROUP + h * 2 * PER_CHUNK + q).reshape(-1)
    goes = (q * hub_fold + h * (hub_fold // HALVES) + p).reshape(-1)
    hub_gather = np.zeros((1, served * GROUP), np.int32)
    hub_gather[0, came] = goes
    hub_scatter = np.full((1, 2 * PER_CHUNK * hub_fold), -1, np.int32)
    hub_scatter[0, goes] = came

    smem = pl.BlockSpec(memory_space=pltpu.SMEM)
    vmem = pl.BlockSpec(memory_space=pltpu.VMEM)
    hbm = pl.BlockSpec(memory_space=pl.ANY)
    parcels = (chunks * count, GROUP, wide)
    return pl.pallas_call(
        functools.partial(layer_kernel, count, float(lat_dev * count * width)),
        out_shape=jax.ShapeDtypeStruct(field.shape, field.dtype),
        in_specs=[smem] * 2 + [vmem] * 12 + [hbm] * 4,
        out_specs=hbm,
        scratch_shapes=[
            pltpu.VMEM(field.shape, BF16),
            pltpu.VMEM((2 * degs, width), BF16),
            pltpu.VMEM(legendre.shape, BF16),
            pltpu.VMEM(mixing.shape, BF16),
            pltpu.VMEM((chunks, rows, width), BF16),
            pltpu.VMEM((chunks, width, rows), BF16),
            pltpu.VMEM(parcels, BF16),
            pltpu.VMEM(parcels, BF16),
            pltpu.VMEM(parcels, BF16),
            pltpu.VMEM(parcels, BF16),
            pltpu.VMEM((slots, degs, nlat), BF16),
            pltpu.VMEM((slots, nlat, degs), BF16),
            pltpu.VMEM((slots, 2 * chans, 2 * chans), BF16),
            pltpu.VMEM((PER_CHUNK, nlat, 2 * chans), BF16),
            pltpu.VMEM((rows, wide), BF16),
            pltpu.VMEM((HALVES, rows, wide), BF16),
            pltpu.VMEM((HALVES, width, wide), F32),
            pltpu.VMEM((chunks, 2 * degs, rows), BF16),
            pltpu.VMEM((2, served, GROUP, wide), BF16),
            pltpu.VMEM((2, served, GROUP, wide), BF16),
            pltpu.VMEM((2, packed, HUB_LATS), BF16),
            pltpu.VMEM((2, packed, HUB_LATS), BF16),
            pltpu.VMEM((2, packed, 2 * chans), BF16),
            pltpu.VMEM((2, packed, 2 * chans), BF16),
            pltpu.VMEM((packed, 2 * chans), BF16),
            pltpu.VMEM((2, packed, 2 * chans), BF16),
            pltpu.VMEM((degs, 2 * chans), F32),
            pltpu.VMEM((PER_CHUNK, degs, 2 * chans), BF16),
            pltpu.VMEM((PER_CHUNK, thirds * hub_fold, 2 * chans), BF16),
            pltpu.VMEM((2 * PER_CHUNK * hub_fold, wide), BF16),
            pltpu.VMEM((2, chans), F32),
            pltpu.VMEM((2, chans), F32),
            pltpu.VMEM((2, chans // 2), F32),
            pltpu.VMEM((count // 2, 2, chans // 2), F32),
            pltpu.VMEM((2, chans // 2), F32),
            pltpu.VMEM((2, chans // 2), F32),
            pltpu.VMEM((2, chans), F32),
            pltpu.SemaphoreType.DMA,
            pltpu.SemaphoreType.DMA((6,)),
            pltpu.SemaphoreType.DMA((chunks,)),
            pltpu.SemaphoreType.DMA((chunks,)),
            pltpu.SemaphoreType.DMA((2,)),
            pltpu.SemaphoreType.DMA((4,)),
            pltpu.SemaphoreType.DMA((4,)),
            pltpu.SemaphoreType.DMA((4,)),
            pltpu.SemaphoreType.DMA((4,)),
            pltpu.SemaphoreType.DMA,
        ],
        compiler_params=pltpu.CompilerParams(
            collective_id=0, has_side_effects=True, vmem_limit_bytes=66_000_000
        ),
        name="layer",
    )(
        slot_wave,
        jnp.asarray(sums),
        slot_wave[None],
        jnp.asarray(slot),
        jnp.asarray(lat_old),
        jnp.asarray(lat_new),
        jnp.asarray(gather),
        jnp.asarray(scatter),
        jnp.asarray(hub_chip),
        jnp.asarray(hub_inner),
        jnp.asarray(hub_lane),
        jnp.asarray(hub_gather),
        jnp.asarray(hub_scatter),
        gain[None],
        field,
        jnp.asarray(cosines),
        legendre,
        mixing,
    )


def solution(mesh):
    return jax.shard_map(
        per_device,
        mesh=mesh,
        in_specs=(
            P(("member", "lat"), None, None),
            P(),
            P(),
            P("lat", None, None),
            P("lat", None, None, None),
        ),
        out_specs=P(("member", "lat"), None, None),
        check_vma=False,
    )
```

```python
import functools
import math

import jax
import jax.numpy as jnp
import numpy as np
from jax import lax
from jax.experimental import pallas as pl
from jax.experimental.pallas import tpu as pltpu
from jax.sharding import PartitionSpec as P

MESH = pl.DeviceIdType.MESH
F32 = jnp.float32
BF16 = jnp.bfloat16
HALVES = 2
PER_CHUNK = 2
GROUP = HALVES * PER_CHUNK * 2
HUB_LATS = 128


def dot(a, b):
    return jnp.dot(a, b, preferred_element_type=F32)


def dot_tn(a, b):
    return lax.dot_general(a, b, (((0,), (0,)), ((), ())), preferred_element_type=F32)


def dot_nt(a, b):
    return lax.dot_general(a, b, (((1,), (1,)), ((), ())), preferred_element_type=F32)


def one_hot(target, rows):
    wide = jnp.broadcast_to(target, (rows, target.shape[1]))
    at = lax.broadcasted_iota(jnp.int32, wide.shape, 0)
    return jnp.where(at == wide, 1.0, 0.0).astype(BF16)


def layer_kernel(
    count,
    total_count,
    wave_ref,
    rowsum_ref,
    wave_row_ref,
    slot_ref,
    lat_old_ref,
    lat_new_ref,
    gather_ref,
    scatter_ref,
    hub_chip_ref,
    hub_inner_ref,
    hub_lane_ref,
    hub_gather_ref,
    hub_scatter_ref,
    pick_ref,
    single_ref,
    gain_ref,
    field_hbm,
    cos_hbm,
    legendre_hbm,
    mixing_hbm,
    out_hbm,
    field_v,
    cos_v,
    legendre_v,
    mixing_v,
    table_v,
    table_t_v,
    out_one,
    in_one,
    out_two,
    in_two,
    leg_v,
    leg_t_v,
    big_v,
    spec_v,
    z_v,
    picked_v,
    acc_v,
    chosen_v,
    hub_in,
    hub_out,
    leg_out,
    leg_in,
    part_out,
    part_in,
    mix_out,
    mix_in,
    coef_v,
    mixed_v,
    hub_spec_v,
    hub_z_v,
    mine_v,
    other_v,
    half_v,
    halves_v,
    total_v,
    rest_v,
    scale_v,
    send_sem,
    stat_sem,
    recv_one,
    recv_two,
    hub_sem,
    leg_sem,
    part_sem,
    mix_sem,
    load_sem,
    store_sem,
):
    me = lax.axis_index("lat")
    lat_dev, width, chans = field_v.shape
    slots, degs, nlat = legendre_v.shape
    thirds = lat_dev // HALVES
    chunks = slots // PER_CHUNK
    rows = count * GROUP
    fold = HALVES * count
    degs_kept = cos_v.shape[0] // 2
    core = lax.rem(me, 2)
    partner = me + 1 - 2 * core
    chip = me // 2
    chips = count // 2
    far = chips // 2
    served = hub_in.shape[1]
    reach = far - (served - 1) // 2
    packed = part_in.shape[1]
    hub_fold = hub_spec_v.shape[1] // thirds
    last = chunks - 1
    near = 2 * (2 * reach - 1)

    def device(at_chip, at_core):
        return 2 * lax.rem(at_chip + 2 * chips, chips) + at_core

    inv_root = 1.0 / math.sqrt(width)
    lat_scale = math.sqrt(nlat / degs)

    barrier = pltpu.get_barrier_semaphore()

    def greet(k, carry):
        pl.semaphore_signal(
            barrier, inc=1, device_id={"lat": lax.rem(me + k, count)}, device_id_type=MESH
        )
        return carry

    in_one[last * count : (last + 1) * count] = jnp.zeros((count, *in_one.shape[1:]), BF16)
    lax.fori_loop(1, count, greet, 0)

    loads = [
        pltpu.make_async_copy(src, dst, load_sem.at[i])
        for i, (src, dst) in enumerate(
            (
                (field_hbm, field_v),
                (cos_hbm, cos_v),
                (legendre_hbm, legendre_v),
                (mixing_hbm, mixing_v),
            )
        )
    ]
    for load in loads:
        load.start()
    loads[0].wait()

    part = width // 10
    local_count = float(lat_dev * width)

    def add_rows(i, total):
        block = field_v[i // 10, pl.ds(pl.multiple_of((i % 10) * part, 16), part), :]
        return total + jnp.sum(block.astype(F32), axis=0, keepdims=True)

    mean_here = lax.fori_loop(0, lat_dev * 10, add_rows, jnp.zeros((1, chans), F32)) / local_count

    def add_squares(i, total):
        block = field_v[i // 10, pl.ds(pl.multiple_of((i % 10) * part, 16), part), :]
        off = block.astype(F32) - mean_here
        return total + jnp.sum(off * off, axis=0, keepdims=True)

    squares_here = lax.fori_loop(0, lat_dev * 10, add_squares, jnp.zeros((1, chans), F32))
    mine_v[0:1, :] = mean_here
    mine_v[1:2, :] = squares_here

    loads[1].wait()
    wave_of_slot = one_hot(wave_row_ref[...][None, :], degs_kept)

    def build_table(k):
        for r in range(2):
            row_slot = one_hot(slot_ref[k, r], wave_row_ref.shape[0])
            chosen_v[k, r * degs_kept : (r + 1) * degs_kept, :] = dot(wave_of_slot, row_slot).astype(
                BF16
            )
        table_v[k] = dot_tn(chosen_v[k], cos_v[...]).astype(BF16)

    row_half = lax.broadcasted_iota(jnp.int32, (rows, chans), 0) // (GROUP // HALVES) % HALVES

    def transform(k):
        offset = dot(table_v[k], jnp.ones((width, 128), BF16))[:, :1] * scale_v[0:1, :]

        def third(t, carry):
            low = dot(table_v[k], field_v[t])
            high = dot(table_v[k], field_v[thirds + t])
            both = (jnp.where(row_half == 0, low, high) - offset) * inv_root
            out_one[
                pl.ds(k * count, count), :, pl.ds(pl.multiple_of(t * chans, 128), chans)
            ] = both.reshape(count, GROUP, chans).astype(BF16)
            return carry

        lax.fori_loop(0, thirds, third, 0)

    def parcel(src, dst, there, recv):
        pltpu.make_async_remote_copy(
            src_ref=src,
            dst_ref=dst,
            send_sem=send_sem,
            recv_sem=recv,
            device_id={"lat": there},
            device_id_type=MESH,
        ).start()

    def send_near(src, dst, recv):
        first = device(chip - (reach - 1), 0)

        def send(i, carry):
            step = lax.rem(2 * (reach - 1) + core + i, near)
            there = lax.rem(first + step, count)
            parcel(src.at[last * count + there], dst.at[last * count + me], there, recv.at[last])
            return carry

        lax.fori_loop(1, near, send, 0)

    def send_to_hubs():
        def block(owner):
            return out_one.at[last * count + owner]

        side_here = 1 - 2 * core
        for to in range(2):
            there = device(chip - side_here * (far - reach), to)
            parcel(
                block(device(chip + far, to)),
                hub_in.at[core, served - 1],
                there,
                hub_sem.at[core],
            )
        for i, side in enumerate((1, -1)):

            def send(v, carry):
                e, to = v // 2, lax.rem(v, 2)
                parcel(
                    block(device(chip - side * (e + reach), to)),
                    hub_in.at[i, 2 * e + core],
                    device(chip - side * e, to),
                    hub_sem.at[i],
                )
                return carry

            lax.fori_loop(2, served - 1, send, 0)
            parcel(
                block(device(chip - side * reach, 1 - core)),
                hub_in.at[i, core],
                partner,
                hub_sem.at[i],
            )
            hub_in[i, core] = out_one[last * count + device(chip - side * reach, core)]

    def send_from_hub(i):
        side = 1 - 2 * i
        owner = device(chip - side * reach, core)
        dst = in_two.at[last * count + owner]

        def send(v, carry):
            there = device(chip + side * (v // 2), lax.rem(v, 2))
            parcel(hub_out.at[i, v], dst, there, recv_two.at[last])
            return carry

        lax.fori_loop(2, served - 1, send, 0)
        parcel(hub_out.at[i, 1 - core], dst, partner, recv_two.at[last])
        there = device(chip + side * (far - reach), i)
        parcel(hub_out.at[i, served - 1], dst, there, recv_two.at[last])
        in_two[last * count + owner] = hub_out[i, core]

    def to_side(src, dst, sems, i, toward):
        return pltpu.make_async_remote_copy(
            src_ref=src,
            dst_ref=dst.at[i],
            send_sem=sems.at[i],
            recv_sem=sems.at[2 + i],
            device_id={"lat": device(chip + toward * (1 - 2 * i) * reach, core)},
            device_id_type=MESH,
        )

    def wave_at(owner, j):
        return wave_ref[owner * slots + last * PER_CHUNK + j]

    def pack(owner, j):
        low = degs - wave_at(owner, 0)
        begin = jnp.where(j == 0, 0, low)
        end = begin + degs - wave_at(owner, j)
        degree = lax.broadcasted_iota(jnp.int32, (degs, packed), 0)
        row = lax.broadcasted_iota(jnp.int32, (degs, packed), 1)
        hit = (degree - row == wave_at(owner, j) - begin) & (row >= begin) & (row < end)
        return jnp.where(hit, 1.0, 0.0).astype(BF16)

    def hub_legendre(i):
        return dot(leg_in[i], one_hot(hub_lane_ref[...], HUB_LATS)).astype(BF16)

    def of_slot(i, j, value):
        low = degs - wave_at(device(chip - (1 - 2 * i) * reach, core), 0)
        row = lax.broadcasted_iota(jnp.int32, value.shape, 0)
        return jnp.where((row < low) == (j == 0), value, 0.0)

    def send_chunk(k, src, dst, recv):
        def send(there):
            pltpu.make_async_remote_copy(
                src_ref=src.at[k * count + there],
                dst_ref=dst.at[k * count + me],
                send_sem=send_sem,
                recv_sem=recv.at[k],
                device_id={"lat": there},
                device_id_type=MESH,
            ).start()

        def both(i, carry):
            step = jnp.where(lax.rem(i, 2) == 0, count // 2 - 1 - i // 2, (i + 1) // 2)
            send(lax.rem(me + step, count))
            send(lax.rem(me + count - step, count))
            return carry

        lax.fori_loop(0, count // 2 - 1, both, 0)
        send(lax.rem(me + count // 2, count))

    def wait_chunk(k, dst, recv, parcels):
        others = dst.at[pl.ds(k * count, parcels)]
        pltpu.make_async_copy(others, others, recv.at[k]).wait()

    def tell(src, dst, sems, there):
        return pltpu.make_async_remote_copy(
            src_ref=src,
            dst_ref=dst,
            send_sem=stat_sem.at[sems],
            recv_sem=stat_sem.at[sems + 1],
            device_id={"lat": there},
            device_id_type=MESH,
        )

    lanes = chans // 2
    def normalise(block, owner, k, j, r, keep):
        wave = jnp.minimum(wave_ref[owner * slots + k * PER_CHUNK + j], degs_kept - 1)
        rowsum = jnp.where(k == 0, 0.0, rowsum_ref[r * degs_kept + wave])
        extra = scale_v[0:1, :] * scale_v[1:2, :] * (-inv_root * rowsum)
        return (block * scale_v[1:2, :] + extra * keep).astype(BF16)

    def hub_forward():
        for sem in (2, 3):
            pltpu.make_async_copy(
                halves_v.at[pl.ds(0, count // 2 - 1)],
                halves_v.at[pl.ds(0, count // 2 - 1)],
                stat_sem.at[sem],
            ).wait()
        means = halves_v[:, 0, :]
        mean_half = jnp.sum(means, axis=0, keepdims=True) / float(count // 2)
        apart = means - mean_half
        total_v[0:1, :] = mean_half
        total_v[1:2, :] = (
            jnp.sum(halves_v[:, 1, :], axis=0, keepdims=True)
            + 2.0 * local_count * jnp.sum(apart * apart, axis=0, keepdims=True)
        ) / total_count
        share = tell(total_v, rest_v, 4, partner)
        share.start()
        share.wait()
        for i in range(2):
            scale_v[i : i + 1, :lanes] = jnp.where(
                core == 0, total_v[i : i + 1, :], rest_v[i : i + 1, :]
            )
            scale_v[i : i + 1, lanes:] = jnp.where(
                core == 0, rest_v[i : i + 1, :], total_v[i : i + 1, :]
            )
        scale_v[1:2, :] = gain_ref[...] / jnp.sqrt(scale_v[1:2, :] + 1e-05)

        def one_side(i, carry):
            to_side(leg_out.at[i], leg_in, leg_sem, i, 1).wait()
            pltpu.make_async_copy(
                hub_in.at[i, pl.ds(0, served - 1)], hub_in.at[i, pl.ds(0, served - 1)], hub_sem.at[i]
            ).wait()
            owner = device(chip - (1 - 2 * i) * reach, core)
            arrived = hub_in[i].reshape(served * GROUP, thirds * chans)
            ordered = dot(one_hot(hub_gather_ref[...], 2 * PER_CHUNK * hub_fold), arrived)
            for q in range(2 * PER_CHUNK):
                j, r = q // 2, q % 2
                for t in range(thirds):
                    block = ordered[q * hub_fold : (q + 1) * hub_fold, t * chans : (t + 1) * chans]
                    hub_spec_v[j, t * hub_fold : (t + 1) * hub_fold, r * chans : (r + 1) * chans] = (
                        normalise(block, owner, last, j, r, 1.0)
                    )
            leg = hub_legendre(i)
            total = of_slot(i, 0, dot(leg, hub_spec_v[0])) + of_slot(i, 1, dot(leg, hub_spec_v[1]))
            part_out[i] = total.astype(BF16)
            to_side(part_out.at[i], part_in, part_sem, i, -1).start()
            return carry

        lax.fori_loop(0, 2, one_side, 0)

    scale_v[...] = jnp.zeros_like(scale_v)
    acc_v[...] = jnp.zeros_like(acc_v)

    build_table(last)
    transform(last)
    loads[2].wait()
    for i, side in enumerate((1, -1)):
        at_chip = lax.rem(chip + side * hub_chip_ref[...] + 2 * chips, chips)
        lats = one_hot(at_chip * (2 * lat_dev) + hub_inner_ref[i], nlat)
        rows_here = jnp.zeros((packed, HUB_LATS), F32)
        for j in range(PER_CHUNK):
            values = dot(legendre_v[last * PER_CHUNK + j], lats).astype(BF16)
            rows_here += dot_tn(pack(me, j), values)
        leg_out[i] = rows_here.astype(BF16)
    pl.semaphore_wait(barrier, count - 1)

    pair = tell(mine_v, other_v, 0, partner)
    pair.start()
    pair.wait()
    gap = mine_v[0:1, :] - other_v[0:1, :]
    pair_mean = (mine_v[0:1, :] + other_v[0:1, :]) * 0.5
    pair_squares = mine_v[1:2, :] + other_v[1:2, :] + (0.5 * local_count) * gap * gap
    half_v[0:1, :] = jnp.where(core == 0, pair_mean[:, :lanes], pair_mean[:, lanes:])
    half_v[1:2, :] = jnp.where(core == 0, pair_squares[:, :lanes], pair_squares[:, lanes:])
    halves_v[me // 2] = half_v[...]

    def send_stats(i, carry):
        tell(half_v, halves_v.at[me // 2], 2, lax.rem(me + 2 * i, count)).start()
        return carry

    lax.fori_loop(1, count // 2, send_stats, 0)
    for i in range(2):
        to_side(leg_out.at[i], leg_in, leg_sem, i, 1).start()
    send_to_hubs()
    send_near(out_one, in_one, recv_one)
    in_one[last * count + me] = out_one[last * count + me]

    def outward(turn, carry):
        k = last - turn
        build_table(k)
        pl.when(k == 0)(hub_forward)
        transform(k)
        send_chunk(k, out_one, in_one, recv_one)
        in_one[k * count + me] = out_one[k * count + me]
        return carry

    lax.fori_loop(1, chunks, outward, 0)

    loads[3].wait()

    def prepare(s, carry):
        leg_v[s] = dot(legendre_v[s], one_hot(lat_old_ref[...], nlat)).astype(BF16)
        leg_t_v[s] = dot_nt(one_hot(lat_new_ref[...], nlat), legendre_v[s]).astype(BF16)
        real = mixing_v[s, 0]
        imag = mixing_v[s, 1]
        big_v[s, :chans, :chans] = real
        big_v[s, :chans, chans:] = imag
        big_v[s, chans:, :chans] = -imag
        big_v[s, chans:, chans:] = real
        return carry

    lax.fori_loop(0, slots, prepare, 0)

    table_row = lax.broadcasted_iota(jnp.int32, (2 * degs_kept, rows // HALVES), 0)
    weight = jnp.where((table_row == 0) | (table_row == degs_kept), 1.0, 2.0)

    def build_table_t(k, carry):
        chosen = (dot(chosen_v[k], one_hot(single_ref[...], rows)) * weight).astype(BF16)
        table_t_v[k] = dot_tn(cos_v[...], chosen).astype(BF16)
        return carry

    lax.fori_loop(0, chunks, build_table_t, 0)

    place = lax.rem(lax.broadcasted_iota(jnp.int32, (fold, chans), 0), count) // 2
    apart_chips = jnp.abs(place - chip)
    close = jnp.minimum(apart_chips, chips - apart_chips) < reach

    def middle(turn, carry):
        k = last - turn

        @pl.when(k == last)
        def _():
            wait_chunk(last, in_one, recv_one, near - 1)
            for i in range(2):
                to_side(part_out.at[i], part_in, part_sem, i, -1).wait()

        @pl.when(k == 0)
        def _():
            def one_side(i, carry):
                to_side(mix_out, mix_in, mix_sem, i, 1).wait()
                leg = hub_legendre(i)
                for j in range(PER_CHUNK):
                    rows_j = of_slot(i, j, mix_in[i].astype(F32)).astype(BF16)
                    back = (dot_tn(leg, rows_j) * lat_scale).astype(BF16)
                    for r in range(2):
                        q = 2 * j + r
                        for t in range(thirds):
                            hub_z_v[
                                q * hub_fold : (q + 1) * hub_fold, t * chans : (t + 1) * chans
                            ] = back[t * hub_fold : (t + 1) * hub_fold, r * chans : (r + 1) * chans]
                home = dot(one_hot(hub_scatter_ref[...], served * GROUP), hub_z_v[...])
                hub_out[i] = home.reshape(served, GROUP, thirds * chans).astype(BF16)
                send_from_hub(i)
                return carry

            lax.fori_loop(0, 2, one_side, 0)

        @pl.when(k != last)
        def _():
            wait_chunk(k, in_one, recv_one, count - 1)

        arrived = in_one[pl.ds(k * count, count)].reshape(rows, thirds * chans)
        ordered = dot(one_hot(gather_ref[...], rows), arrived)
        keep = jnp.where(close | (k != last), 1.0, 0.0)
        for q in range(PER_CHUNK * 2):
            j, r = q // 2, q % 2
            for t in range(thirds):
                block = ordered[q * fold : (q + 1) * fold, t * chans : (t + 1) * chans]
                spec_v[j, t * fold : (t + 1) * fold, r * chans : (r + 1) * chans] = normalise(
                    block, me, k, j, r, keep
                )

        def one_slot(j, carry):
            s = k * PER_CHUNK + j
            coef_v[...] = dot(leg_v[s], spec_v[j])

            @pl.when(k == last)
            def _():
                for i in range(2):
                    coef_v[...] += dot(pack(me, j), part_in[i])

            degree = lax.broadcasted_iota(jnp.int32, coef_v.shape, 0)
            coef = jnp.where(degree >= wave_ref[me * slots + s], coef_v[...], 0.0).astype(BF16)
            mixed_v[j] = dot(coef, big_v[s]).astype(BF16)
            back = (dot(leg_t_v[s], mixed_v[j]) * lat_scale).astype(BF16)
            for r in range(2):
                q = 2 * j + r
                for t in range(thirds):
                    z_v[
                        pl.ds(pl.multiple_of(q * fold, 16), fold), t * chans : (t + 1) * chans
                    ] = back[
                        t * fold : (t + 1) * fold, r * chans : (r + 1) * chans
                    ]
            return carry

        lax.fori_loop(0, PER_CHUNK, one_slot, 0)
        home = dot(one_hot(scatter_ref[...], rows), z_v[...])
        out_two[pl.ds(k * count, count)] = home.reshape(count, GROUP, thirds * chans).astype(BF16)
        in_two[k * count + me] = out_two[k * count + me]

        @pl.when(k == last)
        def _():
            mix_out[...] = (
                dot_tn(pack(me, 0), mixed_v[0]) + dot_tn(pack(me, 1), mixed_v[1])
            ).astype(BF16)
            for i in range(2):
                to_side(mix_out, mix_in, mix_sem, i, 1).start()
            send_near(out_two, in_two, recv_two)

        @pl.when(k != last)
        def _():
            send_chunk(k, out_two, in_two, recv_two)

        return carry

    lax.fori_loop(0, chunks, middle, 0)

    def take(k):
        returned = in_two[pl.ds(k * count, count)].reshape(rows, thirds * chans)
        for h in range(HALVES):
            picked = dot(one_hot(pick_ref[h], rows // HALVES), returned).astype(BF16)
            for t in range(thirds):
                picked_v[h * thirds + t] = picked[:, t * chans : (t + 1) * chans]

    def inner(turn, carry):
        k = last - turn
        pl.when(k == last)(lambda: wait_chunk(last, in_two, recv_two, count - 3))
        pl.when(k != last)(lambda: wait_chunk(k, in_two, recv_two, count - 1))
        take(k)

        def plane(a, carry):
            acc_v[a] += dot(table_t_v[k], picked_v[a])
            return carry

        return lax.fori_loop(0, lat_dev, plane, carry)

    lax.fori_loop(0, chunks - 1, inner, 0)
    wait_chunk(0, in_two, recv_two, count - 1)
    take(0)

    def last_plane(a, carry):
        filtered = (acc_v[a] + dot(table_t_v[0], picked_v[a])) * inv_root
        normed = ((field_v[a].astype(F32) - scale_v[0:1, :]) * scale_v[1:2, :]).astype(BF16)
        field_v[a] = (normed.astype(F32) + filtered).astype(BF16)
        pltpu.make_async_copy(field_v.at[a], out_hbm.at[a], store_sem).start()
        return carry

    lax.fori_loop(0, lat_dev, last_plane, 0)
    pltpu.make_async_copy(field_v, out_hbm, store_sem).wait()
    for amount in [count - 1] * (2 * last) + [near - 1, 2 * (served - 1)] * 2:
        sent = in_one.at[pl.ds(0, amount)]
        pltpu.make_async_copy(sent, sent, send_sem).wait()


def hand_over(src, dst, through, load_sem, store_sem):
    planes = range(src.shape[0])
    loads = [pltpu.make_async_copy(src.at[a], through.at[a], load_sem.at[a]) for a in planes]
    stores = [pltpu.make_async_copy(through.at[a], dst.at[a], store_sem.at[a]) for a in planes]
    for load in loads:
        load.start()
    for load, store in zip(loads, stores):
        load.wait()
        store.start()
    for store in stores:
        store.wait()


def cosine_rows(waves, width):
    points = np.arange(width, dtype=np.int64)[None, :] * np.arange(waves, dtype=np.int64)[:, None]
    phase = (points % width).astype(np.float32) * np.float32(2.0 * math.pi / width)
    return np.concatenate([np.cos(phase), -np.sin(phase)]).astype(jnp.bfloat16)


def per_device(field, gain, slot_wave, legendre, mixing):
    count = lax.axis_size("lat")
    lat_dev, width, chans = field.shape
    slots, degs, nlat = legendre.shape
    thirds = lat_dev // HALVES
    chunks = slots // PER_CHUNK
    rows = count * GROUP
    fold = HALVES * count
    wide = thirds * chans

    cosines = cosine_rows(degs, width)
    sums = np.sum(cosines.astype(np.float64), axis=1).astype(np.float32)
    k, r, d, _, j, part = np.meshgrid(
        np.arange(chunks),
        np.arange(2),
        np.arange(count),
        np.arange(HALVES),
        np.arange(PER_CHUNK),
        np.arange(2),
        indexing="ij",
    )
    slot = np.where(r == part, d * slots + k * PER_CHUNK + j, -1).astype(np.int32)
    slot = slot.reshape(chunks, 2, 1, rows)

    d, h, t = np.meshgrid(np.arange(count), np.arange(HALVES), np.arange(thirds), indexing="ij")
    old = (d * lat_dev + h * thirds + t).reshape(-1)
    new = (t * fold + h * count + d).reshape(-1)
    lat_old = np.zeros((1, nlat), np.int32)
    lat_old[0, new] = old
    lat_new = np.zeros((1, nlat), np.int32)
    lat_new[0, old] = new
    d, h, q = np.meshgrid(
        np.arange(count), np.arange(HALVES), np.arange(2 * PER_CHUNK), indexing="ij"
    )
    came = (d * GROUP + h * 2 * PER_CHUNK + q).reshape(-1)
    goes = (q * fold + h * count + d).reshape(-1)
    gather = np.zeros((1, rows), np.int32)
    gather[0, came] = goes
    scatter = np.zeros((1, rows), np.int32)
    scatter[0, goes] = came

    far = count // 4
    served = 2 * (far - 2) + 1
    while served * lat_dev > HUB_LATS:
        served -= 2
    reach = far - (served - 1) // 2
    hub_fold = HALVES * (-(-served // 8) * 8)
    packed = -(-(2 * degs - (4 * (chunks - 1) + 2) * count + 1) // 8) * 8
    t, h, p = np.meshgrid(
        np.arange(thirds), np.arange(HALVES), np.arange(served), indexing="ij"
    )
    lane = np.arange(t.size)
    hub_chip = np.zeros((1, HUB_LATS), np.int32)
    hub_chip[0, lane] = (reach + p // 2).reshape(-1)
    hub_inner = np.full((2, 1, HUB_LATS), -(2**20), np.int32)
    for i in range(2):
        at_core = np.where(p == served - 1, i, p % 2)
        hub_inner[i, 0, lane] = (at_core * lat_dev + h * thirds + t).reshape(-1)
    hub_lane = np.full((1, thirds * hub_fold), -1, np.int32)
    hub_lane[0, (t * hub_fold + h * (hub_fold // HALVES) + p).reshape(-1)] = lane
    p, h, q = np.meshgrid(
        np.arange(served), np.arange(HALVES), np.arange(2 * PER_CHUNK), indexing="ij"
    )
    came = (p * GROUP + h * 2 * PER_CHUNK + q).reshape(-1)
    goes = (q * hub_fold + h * (hub_fold // HALVES) + p).reshape(-1)
    hub_gather = np.zeros((1, served * GROUP), np.int32)
    hub_gather[0, came] = goes
    hub_scatter = np.full((1, 2 * PER_CHUNK * hub_fold), -1, np.int32)
    hub_scatter[0, goes] = came

    d, h, q = np.meshgrid(
        np.arange(count), np.arange(HALVES), np.arange(2 * PER_CHUNK), indexing="ij"
    )
    pick = np.full((HALVES, 1, rows), -1, np.int32)
    pick[h, 0, d * GROUP + h * 2 * PER_CHUNK + q] = d * 2 * PER_CHUNK + q
    d, q = np.meshgrid(np.arange(count), np.arange(2 * PER_CHUNK), indexing="ij")
    single = (d * GROUP + q).reshape(1, -1).astype(np.int32)

    smem = pl.BlockSpec(memory_space=pltpu.SMEM)
    vmem = pl.BlockSpec(memory_space=pltpu.VMEM)
    hbm = pl.BlockSpec(memory_space=pl.ANY)
    parcels = (chunks * count, GROUP, wide)
    result = pl.pallas_call(
        functools.partial(layer_kernel, count, float(lat_dev * count * width)),
        out_shape=jax.ShapeDtypeStruct(field.shape, field.dtype),
        in_specs=[smem] * 2 + [vmem] * 14 + [hbm] * 4,
        out_specs=hbm,
        scratch_shapes=[
            pltpu.VMEM(field.shape, BF16),
            pltpu.VMEM((2 * degs, width), BF16),
            pltpu.VMEM(legendre.shape, BF16),
            pltpu.VMEM(mixing.shape, BF16),
            pltpu.VMEM((chunks, rows, width), BF16),
            pltpu.VMEM((chunks, width, rows // HALVES), BF16),
            pltpu.VMEM(parcels, BF16),
            pltpu.VMEM(parcels, BF16),
            pltpu.VMEM(parcels, BF16),
            pltpu.VMEM(parcels, BF16),
            pltpu.VMEM((slots, degs, nlat), BF16),
            pltpu.VMEM((slots, nlat, degs), BF16),
            pltpu.VMEM((slots, 2 * chans, 2 * chans), BF16),
            pltpu.VMEM((PER_CHUNK, nlat, 2 * chans), BF16),
            pltpu.VMEM((rows, wide), BF16),
            pltpu.VMEM((lat_dev, rows // HALVES, chans), BF16),
            pltpu.VMEM((lat_dev, width, chans), F32),
            pltpu.VMEM((chunks, 2 * degs, rows), BF16),
            pltpu.VMEM((2, served, GROUP, wide), BF16),
            pltpu.VMEM((2, served, GROUP, wide), BF16),
            pltpu.VMEM((2, packed, HUB_LATS), BF16),
            pltpu.VMEM((2, packed, HUB_LATS), BF16),
            pltpu.VMEM((2, packed, 2 * chans), BF16),
            pltpu.VMEM((2, packed, 2 * chans), BF16),
            pltpu.VMEM((packed, 2 * chans), BF16),
            pltpu.VMEM((2, packed, 2 * chans), BF16),
            pltpu.VMEM((degs, 2 * chans), F32),
            pltpu.VMEM((PER_CHUNK, degs, 2 * chans), BF16),
            pltpu.VMEM((PER_CHUNK, thirds * hub_fold, 2 * chans), BF16),
            pltpu.VMEM((2 * PER_CHUNK * hub_fold, wide), BF16),
            pltpu.VMEM((2, chans), F32),
            pltpu.VMEM((2, chans), F32),
            pltpu.VMEM((2, chans // 2), F32),
            pltpu.VMEM((count // 2, 2, chans // 2), F32),
            pltpu.VMEM((2, chans // 2), F32),
            pltpu.VMEM((2, chans // 2), F32),
            pltpu.VMEM((2, chans), F32),
            pltpu.SemaphoreType.DMA,
            pltpu.SemaphoreType.DMA((6,)),
            pltpu.SemaphoreType.DMA((chunks,)),
            pltpu.SemaphoreType.DMA((chunks,)),
            pltpu.SemaphoreType.DMA((2,)),
            pltpu.SemaphoreType.DMA((4,)),
            pltpu.SemaphoreType.DMA((4,)),
            pltpu.SemaphoreType.DMA((4,)),
            pltpu.SemaphoreType.DMA((4,)),
            pltpu.SemaphoreType.DMA,
        ],
        compiler_params=pltpu.CompilerParams(
            collective_id=0, has_side_effects=True, vmem_limit_bytes=66_000_000
        ),
        name="layer",
    )(
        slot_wave,
        jnp.asarray(sums),
        slot_wave,
        jnp.asarray(slot),
        jnp.asarray(lat_old),
        jnp.asarray(lat_new),
        jnp.asarray(gather),
        jnp.asarray(scatter),
        jnp.asarray(hub_chip),
        jnp.asarray(hub_inner),
        jnp.asarray(hub_lane),
        jnp.asarray(hub_gather),
        jnp.asarray(hub_scatter),
        jnp.asarray(pick),
        jnp.asarray(single),
        gain[None],
        field,
        jnp.asarray(cosines),
        legendre,
        mixing,
    )
    return pl.pallas_call(
        hand_over,
        out_shape=jax.ShapeDtypeStruct(field.shape, field.dtype),
        in_specs=[hbm],
        out_specs=hbm,
        scratch_shapes=[
            pltpu.VMEM(field.shape, BF16),
            pltpu.SemaphoreType.DMA((lat_dev,)),
            pltpu.SemaphoreType.DMA((lat_dev,)),
        ],
        name="result",
    )(result)


def solution(mesh):
    return jax.shard_map(
        per_device,
        mesh=mesh,
        in_specs=(
            P(("member", "lat"), None, None),
            P(),
            P(),
            P("lat", None, None),
            P("lat", None, None, None),
        ),
        out_specs=P(("member", "lat"), None, None),
        check_vma=False,
    )
```

```python
import functools
import math

import jax
import jax.numpy as jnp
import numpy as np
from jax import lax
from jax.experimental import pallas as pl
from jax.experimental.pallas import tpu as pltpu
from jax.sharding import PartitionSpec as P

MESH = pl.DeviceIdType.MESH
F32 = jnp.float32
BF16 = jnp.bfloat16
HALVES = 2
PER_CHUNK = 2
GROUP = HALVES * PER_CHUNK * 2
HUB_LATS = 128


def dot(a, b):
    return jnp.dot(a, b, preferred_element_type=F32)


def dot_tn(a, b):
    return lax.dot_general(a, b, (((0,), (0,)), ((), ())), preferred_element_type=F32)


def dot_nt(a, b):
    return lax.dot_general(a, b, (((1,), (1,)), ((), ())), preferred_element_type=F32)


def one_hot(target, rows):
    wide = jnp.broadcast_to(target, (rows, target.shape[1]))
    at = lax.broadcasted_iota(jnp.int32, wide.shape, 0)
    return jnp.where(at == wide, 1.0, 0.0).astype(BF16)


def layer_kernel(
    count,
    total_count,
    wave_ref,
    rowsum_ref,
    wave_row_ref,
    slot_ref,
    lat_old_ref,
    lat_new_ref,
    gather_ref,
    scatter_ref,
    hub_chip_ref,
    hub_inner_ref,
    hub_lane_ref,
    hub_gather_ref,
    hub_scatter_ref,
    pick_ref,
    single_ref,
    gain_ref,
    field_hbm,
    cos_hbm,
    legendre_hbm,
    mixing_hbm,
    out_hbm,
    field_v,
    cos_v,
    legendre_v,
    mixing_v,
    table_v,
    table_t_v,
    out_one,
    in_one,
    out_two,
    in_two,
    leg_v,
    leg_t_v,
    big_v,
    spec_v,
    z_v,
    picked_v,
    acc_v,
    chosen_v,
    hub_in,
    hub_out,
    leg_out,
    leg_in,
    part_out,
    part_in,
    mix_out,
    mix_in,
    coef_v,
    mixed_v,
    hub_spec_v,
    hub_z_v,
    mine_v,
    other_v,
    half_v,
    halves_v,
    total_v,
    rest_v,
    scale_v,
    send_sem,
    stat_sem,
    recv_one,
    recv_two,
    hub_sem,
    leg_sem,
    part_sem,
    mix_sem,
    load_sem,
    store_sem,
):
    me = lax.axis_index("lat")
    lat_dev, width, chans = field_v.shape
    slots, degs, nlat = legendre_v.shape
    thirds = lat_dev // HALVES
    chunks = slots // PER_CHUNK
    rows = count * GROUP
    fold = HALVES * count
    degs_kept = cos_v.shape[0] // 2
    core = lax.rem(me, 2)
    partner = me + 1 - 2 * core
    chip = me // 2
    chips = count // 2
    far = chips // 2
    served = hub_in.shape[1]
    reach = far - (served - 1) // 2
    packed = part_in.shape[1]
    hub_fold = hub_spec_v.shape[1] // thirds
    last = chunks - 1
    near = 2 * (2 * reach - 1)

    def device(at_chip, at_core):
        return 2 * lax.rem(at_chip + 2 * chips, chips) + at_core

    inv_root = 1.0 / math.sqrt(width)
    lat_scale = math.sqrt(nlat / degs)

    barrier = pltpu.get_barrier_semaphore()

    def greet(k, carry):
        pl.semaphore_signal(
            barrier, inc=1, device_id={"lat": lax.rem(me + k, count)}, device_id_type=MESH
        )
        return carry

    in_one[last * count : (last + 1) * count] = jnp.zeros((count, *in_one.shape[1:]), BF16)
    lax.fori_loop(1, count, greet, 0)

    loads = [
        pltpu.make_async_copy(src, dst, load_sem.at[i])
        for i, (src, dst) in enumerate(
            (
                (field_hbm, field_v),
                (cos_hbm, cos_v),
                (legendre_hbm, legendre_v),
                (mixing_hbm, mixing_v),
            )
        )
    ]
    for load in loads:
        load.start()
    loads[0].wait()

    part = width // 10
    local_count = float(lat_dev * width)

    def add_rows(i, total):
        block = field_v[i // 10, pl.ds(pl.multiple_of((i % 10) * part, 16), part), :]
        return total + jnp.sum(block.astype(F32), axis=0, keepdims=True)

    mean_here = lax.fori_loop(0, lat_dev * 10, add_rows, jnp.zeros((1, chans), F32)) / local_count

    def add_squares(i, total):
        block = field_v[i // 10, pl.ds(pl.multiple_of((i % 10) * part, 16), part), :]
        off = block.astype(F32) - mean_here
        return total + jnp.sum(off * off, axis=0, keepdims=True)

    squares_here = lax.fori_loop(0, lat_dev * 10, add_squares, jnp.zeros((1, chans), F32))
    mine_v[0:1, :] = mean_here
    mine_v[1:2, :] = squares_here

    loads[1].wait()
    wave_of_slot = one_hot(wave_row_ref[...][None, :], degs_kept)

    def build_table(k):
        for r in range(2):
            row_slot = one_hot(slot_ref[k, r], wave_row_ref.shape[0])
            chosen_v[k, r * degs_kept : (r + 1) * degs_kept, :] = dot(wave_of_slot, row_slot).astype(
                BF16
            )
        table_v[k] = dot_tn(chosen_v[k], cos_v[...]).astype(BF16)

    row_half = lax.broadcasted_iota(jnp.int32, (rows, chans), 0) // (GROUP // HALVES) % HALVES

    def transform(k):
        offset = dot(table_v[k], jnp.ones((width, 128), BF16))[:, :1] * scale_v[0:1, :]

        def third(t, carry):
            low = dot(table_v[k], field_v[t])
            high = dot(table_v[k], field_v[thirds + t])
            both = (jnp.where(row_half == 0, low, high) - offset) * inv_root
            out_one[
                pl.ds(k * count, count), :, pl.ds(pl.multiple_of(t * chans, 128), chans)
            ] = both.reshape(count, GROUP, chans).astype(BF16)
            return carry

        lax.fori_loop(0, thirds, third, 0)

    def parcel(src, dst, there, recv):
        pltpu.make_async_remote_copy(
            src_ref=src,
            dst_ref=dst,
            send_sem=send_sem,
            recv_sem=recv,
            device_id={"lat": there},
            device_id_type=MESH,
        ).start()

    def send_near(src, dst, recv):
        first = device(chip - (reach - 1), 0)

        def send(i, carry):
            step = lax.rem(2 * (reach - 1) + core + i, near)
            there = lax.rem(first + step, count)
            parcel(src.at[last * count + there], dst.at[last * count + me], there, recv.at[last])
            return carry

        lax.fori_loop(1, near, send, 0)

    def send_to_hubs():
        def block(owner):
            return out_one.at[last * count + owner]

        side_here = 1 - 2 * core
        for to in range(2):
            there = device(chip - side_here * (far - reach), to)
            parcel(
                block(device(chip + far, to)),
                hub_in.at[core, served - 1],
                there,
                hub_sem.at[core],
            )
        for i, side in enumerate((1, -1)):

            def send(v, carry):
                e, to = v // 2, lax.rem(v, 2)
                parcel(
                    block(device(chip - side * (e + reach), to)),
                    hub_in.at[i, 2 * e + core],
                    device(chip - side * e, to),
                    hub_sem.at[i],
                )
                return carry

            lax.fori_loop(2, served - 1, send, 0)
            parcel(
                block(device(chip - side * reach, 1 - core)),
                hub_in.at[i, core],
                partner,
                hub_sem.at[i],
            )
            hub_in[i, core] = out_one[last * count + device(chip - side * reach, core)]

    def send_from_hub(i):
        side = 1 - 2 * i
        owner = device(chip - side * reach, core)
        dst = in_two.at[last * count + owner]

        def send(v, carry):
            there = device(chip + side * (v // 2), lax.rem(v, 2))
            parcel(hub_out.at[i, v], dst, there, recv_two.at[last])
            return carry

        lax.fori_loop(2, served - 1, send, 0)
        parcel(hub_out.at[i, 1 - core], dst, partner, recv_two.at[last])
        there = device(chip + side * (far - reach), i)
        parcel(hub_out.at[i, served - 1], dst, there, recv_two.at[last])
        in_two[last * count + owner] = hub_out[i, core]

    def to_side(src, dst, sems, i, toward):
        return pltpu.make_async_remote_copy(
            src_ref=src,
            dst_ref=dst.at[i],
            send_sem=sems.at[i],
            recv_sem=sems.at[2 + i],
            device_id={"lat": device(chip + toward * (1 - 2 * i) * reach, core)},
            device_id_type=MESH,
        )

    def wave_at(owner, j):
        return wave_ref[owner * slots + last * PER_CHUNK + j]

    def pack(owner, j):
        low = degs - wave_at(owner, 0)
        begin = jnp.where(j == 0, 0, low)
        end = begin + degs - wave_at(owner, j)
        degree = lax.broadcasted_iota(jnp.int32, (degs, packed), 0)
        row = lax.broadcasted_iota(jnp.int32, (degs, packed), 1)
        hit = (degree - row == wave_at(owner, j) - begin) & (row >= begin) & (row < end)
        return jnp.where(hit, 1.0, 0.0).astype(BF16)

    def hub_legendre(i):
        return dot(leg_in[i], one_hot(hub_lane_ref[...], HUB_LATS)).astype(BF16)

    def of_slot(i, j, value):
        low = degs - wave_at(device(chip - (1 - 2 * i) * reach, core), 0)
        row = lax.broadcasted_iota(jnp.int32, value.shape, 0)
        return jnp.where((row < low) == (j == 0), value, 0.0)

    def send_chunk(k, src, dst, recv):
        def send(there):
            pltpu.make_async_remote_copy(
                src_ref=src.at[k * count + there],
                dst_ref=dst.at[k * count + me],
                send_sem=send_sem,
                recv_sem=recv.at[k],
                device_id={"lat": there},
                device_id_type=MESH,
            ).start()

        def both(i, carry):
            step = jnp.where(lax.rem(i, 2) == 0, count // 2 - 1 - i // 2, (i + 1) // 2)
            send(lax.rem(me + step, count))
            send(lax.rem(me + count - step, count))
            return carry

        lax.fori_loop(0, count // 2 - 1, both, 0)
        send(lax.rem(me + count // 2, count))

    def wait_chunk(k, dst, recv, parcels):
        others = dst.at[pl.ds(k * count, parcels)]
        pltpu.make_async_copy(others, others, recv.at[k]).wait()

    def tell(src, dst, sems, there):
        return pltpu.make_async_remote_copy(
            src_ref=src,
            dst_ref=dst,
            send_sem=stat_sem.at[sems],
            recv_sem=stat_sem.at[sems + 1],
            device_id={"lat": there},
            device_id_type=MESH,
        )

    lanes = chans // 2
    def normalise(block, owner, k, j, r, keep):
        wave = jnp.minimum(wave_ref[owner * slots + k * PER_CHUNK + j], degs_kept - 1)
        rowsum = jnp.where(k == 0, 0.0, rowsum_ref[r * degs_kept + wave])
        extra = scale_v[0:1, :] * scale_v[1:2, :] * (-inv_root * rowsum)
        return (block * scale_v[1:2, :] + extra * keep).astype(BF16)

    def hub_forward():
        for sem in (2, 3):
            pltpu.make_async_copy(
                halves_v.at[pl.ds(0, count // 2 - 1)],
                halves_v.at[pl.ds(0, count // 2 - 1)],
                stat_sem.at[sem],
            ).wait()
        means = halves_v[:, 0, :]
        mean_half = jnp.sum(means, axis=0, keepdims=True) / float(count // 2)
        apart = means - mean_half
        total_v[0:1, :] = mean_half
        total_v[1:2, :] = (
            jnp.sum(halves_v[:, 1, :], axis=0, keepdims=True)
            + 2.0 * local_count * jnp.sum(apart * apart, axis=0, keepdims=True)
        ) / total_count
        share = tell(total_v, rest_v, 4, partner)
        share.start()
        share.wait()
        for i in range(2):
            scale_v[i : i + 1, :lanes] = jnp.where(
                core == 0, total_v[i : i + 1, :], rest_v[i : i + 1, :]
            )
            scale_v[i : i + 1, lanes:] = jnp.where(
                core == 0, rest_v[i : i + 1, :], total_v[i : i + 1, :]
            )
        scale_v[1:2, :] = gain_ref[...] / jnp.sqrt(scale_v[1:2, :] + 1e-05)

        def one_side(i, carry):
            to_side(leg_out.at[i], leg_in, leg_sem, i, 1).wait()
            pltpu.make_async_copy(
                hub_in.at[i, pl.ds(0, served - 1)], hub_in.at[i, pl.ds(0, served - 1)], hub_sem.at[i]
            ).wait()
            owner = device(chip - (1 - 2 * i) * reach, core)
            arrived = hub_in[i].reshape(served * GROUP, thirds * chans)
            ordered = dot(one_hot(hub_gather_ref[...], 2 * PER_CHUNK * hub_fold), arrived)
            for q in range(2 * PER_CHUNK):
                j, r = q // 2, q % 2
                for t in range(thirds):
                    block = ordered[q * hub_fold : (q + 1) * hub_fold, t * chans : (t + 1) * chans]
                    hub_spec_v[j, t * hub_fold : (t + 1) * hub_fold, r * chans : (r + 1) * chans] = (
                        normalise(block, owner, last, j, r, 1.0)
                    )
            leg = hub_legendre(i)
            total = of_slot(i, 0, dot(leg, hub_spec_v[0])) + of_slot(i, 1, dot(leg, hub_spec_v[1]))
            part_out[i] = total.astype(BF16)
            to_side(part_out.at[i], part_in, part_sem, i, -1).start()
            return carry

        lax.fori_loop(0, 2, one_side, 0)

    scale_v[...] = jnp.zeros_like(scale_v)

    build_table(last)
    transform(last)
    pl.semaphore_wait(barrier, count - 1)

    pair = tell(mine_v, other_v, 0, partner)
    pair.start()
    send_to_hubs()
    send_near(out_one, in_one, recv_one)
    in_one[last * count + me] = out_one[last * count + me]
    pair.wait()
    gap = mine_v[0:1, :] - other_v[0:1, :]
    pair_mean = (mine_v[0:1, :] + other_v[0:1, :]) * 0.5
    pair_squares = mine_v[1:2, :] + other_v[1:2, :] + (0.5 * local_count) * gap * gap
    half_v[0:1, :] = jnp.where(core == 0, pair_mean[:, :lanes], pair_mean[:, lanes:])
    half_v[1:2, :] = jnp.where(core == 0, pair_squares[:, :lanes], pair_squares[:, lanes:])
    halves_v[me // 2] = half_v[...]

    def send_stats(i, carry):
        tell(half_v, halves_v.at[me // 2], 2, lax.rem(me + 2 * i, count)).start()
        return carry

    lax.fori_loop(1, count // 2, send_stats, 0)
    loads[2].wait()
    for i, side in enumerate((1, -1)):
        at_chip = lax.rem(chip + side * hub_chip_ref[...] + 2 * chips, chips)
        lats = one_hot(at_chip * (2 * lat_dev) + hub_inner_ref[i], nlat)
        rows_here = jnp.zeros((packed, HUB_LATS), F32)
        for j in range(PER_CHUNK):
            values = dot(legendre_v[last * PER_CHUNK + j], lats).astype(BF16)
            rows_here += dot_tn(pack(me, j), values)
        leg_out[i] = rows_here.astype(BF16)
    for i in range(2):
        to_side(leg_out.at[i], leg_in, leg_sem, i, 1).start()

    def outward(turn, carry):
        k = last - turn
        build_table(k)
        pl.when(k == 0)(hub_forward)
        transform(k)
        send_chunk(k, out_one, in_one, recv_one)
        in_one[k * count + me] = out_one[k * count + me]
        return carry

    lax.fori_loop(1, chunks, outward, 0)
    acc_v[...] = jnp.zeros_like(acc_v)

    loads[3].wait()

    def prepare(s, carry):
        leg_v[s] = dot(legendre_v[s], one_hot(lat_old_ref[...], nlat)).astype(BF16)
        leg_t_v[s] = dot_nt(one_hot(lat_new_ref[...], nlat), legendre_v[s]).astype(BF16)
        real = mixing_v[s, 0]
        imag = mixing_v[s, 1]
        big_v[s, :chans, :chans] = real
        big_v[s, :chans, chans:] = imag
        big_v[s, chans:, :chans] = -imag
        big_v[s, chans:, chans:] = real
        return carry

    lax.fori_loop(0, slots, prepare, 0)

    table_row = lax.broadcasted_iota(jnp.int32, (2 * degs_kept, rows // HALVES), 0)
    weight = jnp.where((table_row == 0) | (table_row == degs_kept), 1.0, 2.0)

    def build_table_t(k, carry):
        chosen = (dot(chosen_v[k], one_hot(single_ref[...], rows)) * weight).astype(BF16)
        table_t_v[k] = dot_tn(cos_v[...], chosen).astype(BF16)
        return carry

    lax.fori_loop(0, chunks, build_table_t, 0)

    place = lax.rem(lax.broadcasted_iota(jnp.int32, (fold, chans), 0), count) // 2
    apart_chips = jnp.abs(place - chip)
    close = jnp.minimum(apart_chips, chips - apart_chips) < reach

    def middle(turn, carry):
        k = last - turn

        @pl.when(k == last)
        def _():
            wait_chunk(last, in_one, recv_one, near - 1)
            for i in range(2):
                to_side(part_out.at[i], part_in, part_sem, i, -1).wait()

        @pl.when(k == 0)
        def _():
            def one_side(i, carry):
                to_side(mix_out, mix_in, mix_sem, i, 1).wait()
                leg = hub_legendre(i)
                for j in range(PER_CHUNK):
                    rows_j = of_slot(i, j, mix_in[i].astype(F32)).astype(BF16)
                    back = (dot_tn(leg, rows_j) * lat_scale).astype(BF16)
                    for r in range(2):
                        q = 2 * j + r
                        for t in range(thirds):
                            hub_z_v[
                                q * hub_fold : (q + 1) * hub_fold, t * chans : (t + 1) * chans
                            ] = back[t * hub_fold : (t + 1) * hub_fold, r * chans : (r + 1) * chans]
                home = dot(one_hot(hub_scatter_ref[...], served * GROUP), hub_z_v[...])
                hub_out[i] = home.reshape(served, GROUP, thirds * chans).astype(BF16)
                send_from_hub(i)
                return carry

            lax.fori_loop(0, 2, one_side, 0)

        @pl.when(k != last)
        def _():
            wait_chunk(k, in_one, recv_one, count - 1)

        arrived = in_one[pl.ds(k * count, count)].reshape(rows, thirds * chans)
        ordered = dot(one_hot(gather_ref[...], rows), arrived)
        keep = jnp.where(close | (k != last), 1.0, 0.0)
        for q in range(PER_CHUNK * 2):
            j, r = q // 2, q % 2
            for t in range(thirds):
                block = ordered[q * fold : (q + 1) * fold, t * chans : (t + 1) * chans]
                spec_v[j, t * fold : (t + 1) * fold, r * chans : (r + 1) * chans] = normalise(
                    block, me, k, j, r, keep
                )

        def one_slot(j, carry):
            s = k * PER_CHUNK + j
            coef_v[...] = dot(leg_v[s], spec_v[j])

            @pl.when(k == last)
            def _():
                for i in range(2):
                    coef_v[...] += dot(pack(me, j), part_in[i])

            degree = lax.broadcasted_iota(jnp.int32, coef_v.shape, 0)
            coef = jnp.where(degree >= wave_ref[me * slots + s], coef_v[...], 0.0).astype(BF16)
            mixed_v[j] = dot(coef, big_v[s]).astype(BF16)
            back = (dot(leg_t_v[s], mixed_v[j]) * lat_scale).astype(BF16)
            for r in range(2):
                q = 2 * j + r
                for t in range(thirds):
                    z_v[
                        pl.ds(pl.multiple_of(q * fold, 16), fold), t * chans : (t + 1) * chans
                    ] = back[
                        t * fold : (t + 1) * fold, r * chans : (r + 1) * chans
                    ]
            return carry

        lax.fori_loop(0, PER_CHUNK, one_slot, 0)
        home = dot(one_hot(scatter_ref[...], rows), z_v[...])
        out_two[pl.ds(k * count, count)] = home.reshape(count, GROUP, thirds * chans).astype(BF16)
        in_two[k * count + me] = out_two[k * count + me]

        @pl.when(k == last)
        def _():
            mix_out[...] = (
                dot_tn(pack(me, 0), mixed_v[0]) + dot_tn(pack(me, 1), mixed_v[1])
            ).astype(BF16)
            for i in range(2):
                to_side(mix_out, mix_in, mix_sem, i, 1).start()
            send_near(out_two, in_two, recv_two)

        @pl.when(k != last)
        def _():
            send_chunk(k, out_two, in_two, recv_two)

        return carry

    lax.fori_loop(0, chunks, middle, 0)

    def take(k):
        returned = in_two[pl.ds(k * count, count)].reshape(rows, thirds * chans)
        for h in range(HALVES):
            picked = dot(one_hot(pick_ref[h], rows // HALVES), returned).astype(BF16)
            for t in range(thirds):
                picked_v[h * thirds + t] = picked[:, t * chans : (t + 1) * chans]

    def inner(turn, carry):
        k = last - turn
        pl.when(k == last)(lambda: wait_chunk(last, in_two, recv_two, count - 3))
        pl.when(k != last)(lambda: wait_chunk(k, in_two, recv_two, count - 1))
        take(k)

        def plane(a, carry):
            acc_v[a] += dot(table_t_v[k], picked_v[a])
            return carry

        return lax.fori_loop(0, lat_dev, plane, carry)

    lax.fori_loop(0, chunks - 1, inner, 0)
    wait_chunk(0, in_two, recv_two, count - 1)
    take(0)

    def last_plane(a, carry):
        filtered = (acc_v[a] + dot(table_t_v[0], picked_v[a])) * inv_root
        normed = ((field_v[a].astype(F32) - scale_v[0:1, :]) * scale_v[1:2, :]).astype(BF16)
        field_v[a] = (normed.astype(F32) + filtered).astype(BF16)
        pltpu.make_async_copy(field_v.at[a], out_hbm.at[a], store_sem).start()
        return carry

    lax.fori_loop(0, lat_dev, last_plane, 0)
    pltpu.make_async_copy(field_v, out_hbm, store_sem).wait()
    for amount in [count - 1] * (2 * last) + [near - 1, 2 * (served - 1)] * 2:
        sent = in_one.at[pl.ds(0, amount)]
        pltpu.make_async_copy(sent, sent, send_sem).wait()


def hand_over(src, dst, through, load_sem, store_sem):
    planes = range(src.shape[0])
    loads = [pltpu.make_async_copy(src.at[a], through.at[a], load_sem.at[a]) for a in planes]
    stores = [pltpu.make_async_copy(through.at[a], dst.at[a], store_sem.at[a]) for a in planes]
    for load in loads:
        load.start()
    for load, store in zip(loads, stores):
        load.wait()
        store.start()
    for store in stores:
        store.wait()


def cosine_rows(waves, width):
    points = np.arange(width, dtype=np.int64)[None, :] * np.arange(waves, dtype=np.int64)[:, None]
    phase = (points % width).astype(np.float32) * np.float32(2.0 * math.pi / width)
    return np.concatenate([np.cos(phase), -np.sin(phase)]).astype(jnp.bfloat16)


def per_device(field, gain, slot_wave, legendre, mixing):
    count = lax.axis_size("lat")
    lat_dev, width, chans = field.shape
    slots, degs, nlat = legendre.shape
    thirds = lat_dev // HALVES
    chunks = slots // PER_CHUNK
    rows = count * GROUP
    fold = HALVES * count
    wide = thirds * chans

    cosines = cosine_rows(degs, width)
    sums = np.sum(cosines.astype(np.float64), axis=1).astype(np.float32)
    k, r, d, _, j, part = np.meshgrid(
        np.arange(chunks),
        np.arange(2),
        np.arange(count),
        np.arange(HALVES),
        np.arange(PER_CHUNK),
        np.arange(2),
        indexing="ij",
    )
    slot = np.where(r == part, d * slots + k * PER_CHUNK + j, -1).astype(np.int32)
    slot = slot.reshape(chunks, 2, 1, rows)

    d, h, t = np.meshgrid(np.arange(count), np.arange(HALVES), np.arange(thirds), indexing="ij")
    old = (d * lat_dev + h * thirds + t).reshape(-1)
    new = (t * fold + h * count + d).reshape(-1)
    lat_old = np.zeros((1, nlat), np.int32)
    lat_old[0, new] = old
    lat_new = np.zeros((1, nlat), np.int32)
    lat_new[0, old] = new
    d, h, q = np.meshgrid(
        np.arange(count), np.arange(HALVES), np.arange(2 * PER_CHUNK), indexing="ij"
    )
    came = (d * GROUP + h * 2 * PER_CHUNK + q).reshape(-1)
    goes = (q * fold + h * count + d).reshape(-1)
    gather = np.zeros((1, rows), np.int32)
    gather[0, came] = goes
    scatter = np.zeros((1, rows), np.int32)
    scatter[0, goes] = came

    far = count // 4
    served = 2 * (far - 2) + 1
    while served * lat_dev > HUB_LATS:
        served -= 2
    reach = far - (served - 1) // 2
    hub_fold = HALVES * (-(-served // 8) * 8)
    packed = -(-(2 * degs - (4 * (chunks - 1) + 2) * count + 1) // 8) * 8
    t, h, p = np.meshgrid(
        np.arange(thirds), np.arange(HALVES), np.arange(served), indexing="ij"
    )
    lane = np.arange(t.size)
    hub_chip = np.zeros((1, HUB_LATS), np.int32)
    hub_chip[0, lane] = (reach + p // 2).reshape(-1)
    hub_inner = np.full((2, 1, HUB_LATS), -(2**20), np.int32)
    for i in range(2):
        at_core = np.where(p == served - 1, i, p % 2)
        hub_inner[i, 0, lane] = (at_core * lat_dev + h * thirds + t).reshape(-1)
    hub_lane = np.full((1, thirds * hub_fold), -1, np.int32)
    hub_lane[0, (t * hub_fold + h * (hub_fold // HALVES) + p).reshape(-1)] = lane
    p, h, q = np.meshgrid(
        np.arange(served), np.arange(HALVES), np.arange(2 * PER_CHUNK), indexing="ij"
    )
    came = (p * GROUP + h * 2 * PER_CHUNK + q).reshape(-1)
    goes = (q * hub_fold + h * (hub_fold // HALVES) + p).reshape(-1)
    hub_gather = np.zeros((1, served * GROUP), np.int32)
    hub_gather[0, came] = goes
    hub_scatter = np.full((1, 2 * PER_CHUNK * hub_fold), -1, np.int32)
    hub_scatter[0, goes] = came

    d, h, q = np.meshgrid(
        np.arange(count), np.arange(HALVES), np.arange(2 * PER_CHUNK), indexing="ij"
    )
    pick = np.full((HALVES, 1, rows), -1, np.int32)
    pick[h, 0, d * GROUP + h * 2 * PER_CHUNK + q] = d * 2 * PER_CHUNK + q
    d, q = np.meshgrid(np.arange(count), np.arange(2 * PER_CHUNK), indexing="ij")
    single = (d * GROUP + q).reshape(1, -1).astype(np.int32)

    smem = pl.BlockSpec(memory_space=pltpu.SMEM)
    vmem = pl.BlockSpec(memory_space=pltpu.VMEM)
    hbm = pl.BlockSpec(memory_space=pl.ANY)
    parcels = (chunks * count, GROUP, wide)
    result = pl.pallas_call(
        functools.partial(layer_kernel, count, float(lat_dev * count * width)),
        out_shape=jax.ShapeDtypeStruct(field.shape, field.dtype),
        in_specs=[smem] * 2 + [vmem] * 14 + [hbm] * 4,
        out_specs=hbm,
        scratch_shapes=[
            pltpu.VMEM(field.shape, BF16),
            pltpu.VMEM((2 * degs, width), BF16),
            pltpu.VMEM(legendre.shape, BF16),
            pltpu.VMEM(mixing.shape, BF16),
            pltpu.VMEM((chunks, rows, width), BF16),
            pltpu.VMEM((chunks, width, rows // HALVES), BF16),
            pltpu.VMEM(parcels, BF16),
            pltpu.VMEM(parcels, BF16),
            pltpu.VMEM(parcels, BF16),
            pltpu.VMEM(parcels, BF16),
            pltpu.VMEM((slots, degs, nlat), BF16),
            pltpu.VMEM((slots, nlat, degs), BF16),
            pltpu.VMEM((slots, 2 * chans, 2 * chans), BF16),
            pltpu.VMEM((PER_CHUNK, nlat, 2 * chans), BF16),
            pltpu.VMEM((rows, wide), BF16),
            pltpu.VMEM((lat_dev, rows // HALVES, chans), BF16),
            pltpu.VMEM((lat_dev, width, chans), F32),
            pltpu.VMEM((chunks, 2 * degs, rows), BF16),
            pltpu.VMEM((2, served, GROUP, wide), BF16),
            pltpu.VMEM((2, served, GROUP, wide), BF16),
            pltpu.VMEM((2, packed, HUB_LATS), BF16),
            pltpu.VMEM((2, packed, HUB_LATS), BF16),
            pltpu.VMEM((2, packed, 2 * chans), BF16),
            pltpu.VMEM((2, packed, 2 * chans), BF16),
            pltpu.VMEM((packed, 2 * chans), BF16),
            pltpu.VMEM((2, packed, 2 * chans), BF16),
            pltpu.VMEM((degs, 2 * chans), F32),
            pltpu.VMEM((PER_CHUNK, degs, 2 * chans), BF16),
            pltpu.VMEM((PER_CHUNK, thirds * hub_fold, 2 * chans), BF16),
            pltpu.VMEM((2 * PER_CHUNK * hub_fold, wide), BF16),
            pltpu.VMEM((2, chans), F32),
            pltpu.VMEM((2, chans), F32),
            pltpu.VMEM((2, chans // 2), F32),
            pltpu.VMEM((count // 2, 2, chans // 2), F32),
            pltpu.VMEM((2, chans // 2), F32),
            pltpu.VMEM((2, chans // 2), F32),
            pltpu.VMEM((2, chans), F32),
            pltpu.SemaphoreType.DMA,
            pltpu.SemaphoreType.DMA((6,)),
            pltpu.SemaphoreType.DMA((chunks,)),
            pltpu.SemaphoreType.DMA((chunks,)),
            pltpu.SemaphoreType.DMA((2,)),
            pltpu.SemaphoreType.DMA((4,)),
            pltpu.SemaphoreType.DMA((4,)),
            pltpu.SemaphoreType.DMA((4,)),
            pltpu.SemaphoreType.DMA((4,)),
            pltpu.SemaphoreType.DMA,
        ],
        compiler_params=pltpu.CompilerParams(
            collective_id=0, has_side_effects=True, vmem_limit_bytes=66_000_000
        ),
        name="layer",
    )(
        slot_wave,
        jnp.asarray(sums),
        slot_wave,
        jnp.asarray(slot),
        jnp.asarray(lat_old),
        jnp.asarray(lat_new),
        jnp.asarray(gather),
        jnp.asarray(scatter),
        jnp.asarray(hub_chip),
        jnp.asarray(hub_inner),
        jnp.asarray(hub_lane),
        jnp.asarray(hub_gather),
        jnp.asarray(hub_scatter),
        jnp.asarray(pick),
        jnp.asarray(single),
        gain[None],
        field,
        jnp.asarray(cosines),
        legendre,
        mixing,
    )
    return pl.pallas_call(
        hand_over,
        out_shape=jax.ShapeDtypeStruct(field.shape, field.dtype),
        in_specs=[hbm],
        out_specs=hbm,
        scratch_shapes=[
            pltpu.VMEM(field.shape, BF16),
            pltpu.SemaphoreType.DMA((lat_dev,)),
            pltpu.SemaphoreType.DMA((lat_dev,)),
        ],
        name="result",
    )(result)


def solution(mesh):
    return jax.shard_map(
        per_device,
        mesh=mesh,
        in_specs=(
            P(("member", "lat"), None, None),
            P(),
            P(),
            P("lat", None, None),
            P("lat", None, None, None),
        ),
        out_specs=P(("member", "lat"), None, None),
        check_vma=False,
    )
```
